256 devices in a mesh: grp: 8 (over y_hi, x), slab: 32 (over z, y_lo, core).
Axes of the slice: x: 4, y: 4 (y_hi: 2, y_lo: 2; y = y_hi * 2 + y_lo), z: 8, core: 2. Of those that a mesh axis runs over, the one named last changes fastest.
Arguments:
- source: float32 [256, 32, 4096], P('grp', None, 'slab'), may hold values from -6 to 6
- occupancy: int32 [32, 4, 512], P('grp', None, 'slab'), may hold values 0 or 1
- classes: int32 [32, 4, 512], P('grp', None, 'slab'), may hold values from 0 to 15
- screen_table: float32 [16], replicated, may hold values from 0.5 to 8
- parents: int32 [16, 2, 256], P('grp', None, 'slab'), may hold values from 0 to 127, as said below
- coarse: float32 [8, 128, 512], P('grp', 'slab'), may hold values from -6 to 6
Outputs:
- middle_field: float32 [128, 16, 2048], P('grp', None, 'slab')
- finest_field: float32 [256, 32, 4096], P('grp', None, 'slab')
The draws below stay inside these ranges and needn't reach their ends.
Inputs may be any that keep to these rules, and one draw needn't show every extreme that they name: parents[I, J, K] is the position, in the list of the group that holds the brick, of the depth-12 brick containing depth-13 brick (I, J, K); each group's list holds each depth-12 brick of the group's region once, so each position is the parent of eight depth-13 bricks. The parent of a brick on slab index s lies in list positions [(s - 1) * 4, (s + 2) * 4).
All inputs are finite; a program needn't handle non-finite values. No bound on the sum of `occupancy` on one device may be relied on, other than what follows from the above.
Results may differ from the reference program's by a relative error of at most 0.00002.
Values sent between devices are 32-bit elements; how exact they have to be, the bound alone decides.
No kernel may reach another device: no remote copies, remote signals or barrier semaphores. Data moves between devices by JAX's collectives and lax.ppermute only.
A program may use at most 128 MiB of HBM per device.

```python
import math
import jax
import jax.numpy as jnp
from jax import lax

BRICK = 8
SWEEPS = 3
CLASSES = 16
CX = 32
NY = 32
CZ = 128
NX = 256
NZ = 4096
LIST = 128
N_GRP = 8
N_SLAB = 32


def draw_parents(key, part):
    groups_x = CX // (4 * BRICK)
    groups_y = NY // (4 * BRICK)
    groups_z = CZ // (4 * BRICK)
    shard_len = groups_x * groups_y * groups_z
    total = shard_len * N_SLAB

    def one_group(group_key):
        first_key, second_key = jax.random.split(group_key)
        offset = jax.random.randint(first_key, (), 1, shard_len, dtype=jnp.int32)
        indices = jnp.arange(total, dtype=jnp.int32)
        segment = (indices - offset + shard_len) // shard_len
        shuffle = jax.random.permutation(second_key, total).astype(jnp.int32)
        placed = jnp.argsort(segment * total + shuffle, stable=True)
        return placed.astype(jnp.int32)
    keys = jax.random.split(jax.random.fold_in(key, 11), N_GRP)
    placement = jax.vmap(one_group)(keys)
    count_x = NX // (2 * BRICK)
    count_y = NY // (2 * BRICK)
    count_z = NZ // (2 * BRICK)
    index_x = jnp.arange(count_x, dtype=jnp.int32)[:, None, None]
    index_y = jnp.arange(count_y, dtype=jnp.int32)[None, :, None]
    index_z = jnp.arange(count_z, dtype=jnp.int32)[None, None, :]
    group = index_x // (CX // (2 * BRICK))
    within_x = index_x % (CX // (2 * BRICK)) // 2
    coarse_y = index_y // 2
    coarse_z = index_z // 2
    slab_index = coarse_z // groups_z
    within_z = coarse_z % groups_z
    geometric = ((slab_index * groups_x + within_x) * groups_y + coarse_y) * groups_z + within_z
    group_full = jnp.broadcast_to(group, (count_x, count_y, count_z))
    geometric_full = jnp.broadcast_to(geometric, (count_x, count_y, count_z))
    return placement[group_full, geometric_full].astype(jnp.int32)


def plant(values, stream_key, least, largest):
    shape = values.shape
    index_at = [jax.random.randint(jax.random.fold_in(stream_key, axis), (), 0, shape[axis]) for axis in range(len(shape))]
    values = values.at[tuple(index_at)].set(least)
    longest = shape.index(max(shape))
    index_at[longest] = (index_at[longest] + 1) % shape[longest]
    return values.at[tuple(index_at)].set(largest)


def level_of(own_key, dims, cuts, low, high):
    def one(dim, blocks):
        heights = jax.random.uniform(jax.random.fold_in(jax.random.fold_in(own_key, 6), dim), (blocks,), jnp.float32, low / len(cuts), high / len(cuts))
        return jnp.repeat(jnp.exp(heights), dims[dim] // blocks).reshape((-1,) + (1,) * (len(dims) - dim - 1))

    factor_of = one(*cuts[0])
    for cut in cuts[1:]:
        factor_of = factor_of * one(*cut)
    return factor_of


def gaussian(rng, dims, scale, most, shards=(), held_as=jnp.bfloat16):
    entries = scale * jax.random.normal(rng, dims, jnp.float32)
    if shards:
        entries = entries * level_of(rng, dims, shards, -0.22, 0.18)
    return jnp.clip(entries, -most, most).astype(held_as)


def setup_inputs(seed: int = 0) -> dict:
    arg_keys = jax.random.split(jax.random.key(seed), 7)
    return {
        "source": gaussian(arg_keys[0], (NX, NY, NZ), 1.0, 6.0, ((0, 8), (2, 32)), jnp.float32),
        "occupancy": plant((jax.random.randint(arg_keys[1], (NX // BRICK, NY // BRICK, NZ // BRICK), 0, 4) < 3).astype(jnp.int32), jax.random.fold_in(arg_keys[1], 1), 0, 1),
        "classes": plant(jax.random.randint(arg_keys[2], (NX // BRICK, NY // BRICK, NZ // BRICK), 0, CLASSES), jax.random.fold_in(arg_keys[2], 1), 0, CLASSES - 1).astype(jnp.int32),
        "screen_table": jnp.clip(jnp.exp(jax.random.uniform(arg_keys[3], (CLASSES,), jnp.float32, math.log(0.5), math.log(8.0))), 0.5, 8.0),
        "parents": draw_parents(jax.random.fold_in(arg_keys[6], 71), 0),
        "coarse": gaussian(arg_keys[5], (N_GRP, LIST, BRICK ** 3), 1.0, 6.0, ((0, 8), (1, 32)), jnp.float32),
    }


screen_strength = 4.0
relaxation = 2.0 / 3.0
stiff_diagonal = 8.0 / 3.0
mass_diagonal = 8.0 / 27.0


def expand(values, factor):
    first, second, third = values.shape
    wide = jnp.broadcast_to(values[:, None, :, None, :, None], (first, factor, second, factor, third, factor))
    return wide.reshape(first * factor, second * factor, third * factor)


def mass_along(values, along):
    length = values.shape[along]
    lower = lax.slice_in_dim(values, 0, length - 2, axis=along)
    middle = lax.slice_in_dim(values, 1, length - 1, axis=along)
    upper = lax.slice_in_dim(values, 2, length, axis=along)
    return (lower + 4.0 * middle + upper) / 6.0


def stiff_along(values, along):
    length = values.shape[along]
    lower = lax.slice_in_dim(values, 0, length - 2, axis=along)
    middle = lax.slice_in_dim(values, 1, length - 1, axis=along)
    upper = lax.slice_in_dim(values, 2, length, axis=along)
    return 2.0 * middle - lower - upper


def relax_step(padded, source, inverse, screen):
    padded_all = jnp.pad(padded, ((0, 0), (1, 1), (0, 0)))
    mass_z = mass_along(padded_all, 2)
    stiff_z = stiff_along(padded_all, 2)
    mass_yz = mass_along(mass_z, 1)
    mixed = stiff_along(mass_z, 1) + mass_along(stiff_z, 1)
    laplace = stiff_along(mass_yz, 0) + mass_along(mixed, 0)
    mass_all = mass_along(mass_yz, 0)
    center = padded[1:-1, :, 1:-1]
    return center + relaxation * inverse * (source - laplace - screen * mass_all)


def sweep_level(field, source, screen_brick, inverse_brick, spread, extent):
    padded = jnp.pad(field, ((1, 1), (0, 0), (1, 1)))
    bricks = extent // spread

    def one_group(column):
        part = lax.dynamic_slice_in_dim(padded, column * extent, extent + 2, 0)
        right = lax.dynamic_slice_in_dim(source, column * extent, extent, 0)
        screen = expand(lax.dynamic_slice_in_dim(screen_brick, column * bricks, bricks, 0), spread)
        inverse = expand(lax.dynamic_slice_in_dim(inverse_brick, column * bricks, bricks, 0), spread)
        return relax_step(part, right, inverse, screen)

    result = lax.map(one_group, jnp.arange(N_GRP, dtype=jnp.int32))
    return result.reshape(field.shape)


def lift(brick_rows, count_x, count_y, count_z):
    half = BRICK // 2
    cells = brick_rows.reshape(count_x, count_y, count_z, 2, half, 2, half, 2, half)
    pairs = jnp.arange(2, dtype=jnp.int32)
    pick_x = ((jnp.arange(count_x, dtype=jnp.int32) % 2)[:, None] == pairs).astype(jnp.float32)
    pick_y = ((jnp.arange(count_y, dtype=jnp.int32) % 2)[:, None] == pairs).astype(jnp.float32)
    pick_z = ((jnp.arange(count_z, dtype=jnp.int32) % 2)[:, None] == pairs).astype(jnp.float32)
    chosen = jnp.sum(cells * pick_x[:, None, None, :, None, None, None, None, None], axis=3)
    chosen = jnp.sum(chosen * pick_y[None, :, None, None, :, None, None, None], axis=4)
    chosen = jnp.sum(chosen * pick_z[None, None, :, None, None, :, None], axis=5)
    fine = jnp.broadcast_to(chosen[:, :, :, :, None, :, None, :, None], (count_x, count_y, count_z, half, 2, half, 2, half, 2))
    fine = fine.reshape(count_x, count_y, count_z, BRICK, BRICK, BRICK)
    return fine.transpose(0, 3, 1, 4, 2, 5).reshape(count_x * BRICK, count_y * BRICK, count_z * BRICK)


def reference(source, occupancy, classes, screen_table, parents, coarse):
    occupied = occupancy.astype(jnp.float32)
    labels = jnp.arange(CLASSES, dtype=jnp.int32)
    weight = jnp.sum(jnp.where(classes[..., None] == labels, screen_table, 0.0), axis=-1)
    screen_brick = screen_strength * weight
    inverse_brick = occupied / (stiff_diagonal + screen_brick * mass_diagonal)
    count_x, count_y, count_z = parents.shape
    group = jnp.arange(count_x, dtype=jnp.int32) // (CX // (2 * BRICK))
    flat = coarse.reshape(N_GRP * LIST, BRICK ** 3)
    position = (group[:, None, None] * LIST + parents).reshape(-1)
    brick_rows = jnp.take(flat, position, axis=0)
    middle_field = lift(brick_rows, count_x, count_y, count_z) * expand(occupied, BRICK // 2)
    size_x, size_y, size_z = source.shape
    source_mid = 0.25 * source.reshape(size_x // 2, 2, size_y // 2, 2, size_z // 2, 2).sum(axis=(1, 3, 5))
    for sweep_index in range(SWEEPS):
        middle_field = sweep_level(middle_field, source_mid, screen_brick, inverse_brick, BRICK // 2, CX // 2)
    finest_field = expand(middle_field, 2) * expand(occupied, BRICK)
    for sweep_index in range(SWEEPS):
        finest_field = sweep_level(finest_field, source, screen_brick, inverse_brick, BRICK, CX)
    return middle_field, finest_field
```

```python
import jax
import jax.numpy as jnp
from jax import lax
from jax.experimental import pallas as pl
from jax.experimental.pallas import tpu as pltpu
from jax.sharding import PartitionSpec as P

BRICK = 8
SWEEPS = 3

screen_strength = 4.0
relaxation = 2.0 / 3.0
stiff_diagonal = 8.0 / 3.0
mass_diagonal = 8.0 / 27.0

F32 = jnp.float32
HI = lax.Precision.HIGHEST
VMEM = pltpu.VMEM
SMEM = pltpu.SMEM

CX, NY, CZ = 32, 32, 128
LANES = 128
COARSE = 4
UNROLL = 8

Z_COARSE, Z_POS, Z_BRICK, Z_SRC, Z_ROWS = 0, 16, 24, 56, 120
X_START, X_MID, X_FINE, X_GHOST, X_BRICK, X_ROWS = 0, 48, 112, 176, 184, 200


def iota(shape, dim):
    return lax.broadcasted_iota(jnp.int32, shape, dim)


def onehot(mask):
    return jnp.where(mask, 1.0, 0.0).astype(F32)


def dot(a, b):
    return jnp.dot(a, b, precision=HI, preferred_element_type=F32)


def turn(v, shift):
    shift = shift % LANES
    return v if shift == 0 else pltpu.roll(v, shift, v.ndim - 1)


def pack_z(src, occ, cls, tab, par, co, zl, zr, pown):
    first = (lax.axis_index("slab") - 1) * COARSE
    for t in range(4):
        part = co[0, :, LANES * t : LANES * (t + 1)]
        zl[Z_COARSE + 4 * t : Z_COARSE + 4 * t + 4, :] = part
        zr[Z_COARSE + 4 * t : Z_COARSE + 4 * t + 4, :] = part
    zl[Z_POS : Z_POS + 8, :] = jnp.full((8, LANES), par[0, 0, 0] - first, jnp.int32).astype(F32)
    zr[Z_POS : Z_POS + 8, :] = jnp.full((8, LANES), par[0, 0, 7] - first, jnp.int32).astype(F32)
    pown[...] = jnp.zeros((32, LANES), F32)
    for bx in range(4):
        occupied = occ[bx].astype(F32)
        labels = cls[bx]
        weight = jnp.zeros((4, 16), F32)
        for c in range(16):
            weight = weight + jnp.where(labels == c, tab[c], 0.0)
        screen = screen_strength * weight
        pown[4 * bx : 4 * bx + 4, 0:16] = occupied / (stiff_diagonal + screen * mass_diagonal)
        pown[16 + 4 * bx : 20 + 4 * bx, 0:16] = screen
    bricks = pown[...]
    lane = iota((32, LANES), 1)
    zl[Z_BRICK : Z_BRICK + 32, :] = jnp.where((lane == 16) | (lane == 17), turn(bricks, 16), 0.0)
    zr[Z_BRICK : Z_BRICK + 32, :] = jnp.where(lane >= 126, turn(bricks, 112), 0.0)
    slot = iota((NY, LANES), 1) // 8
    for g in range(2):
        left = jnp.zeros((NY, LANES), F32)
        right = jnp.zeros((NY, LANES), F32)
        for i in range(16):
            v = src[16 * g + i]
            left = jnp.where(slot == i, turn(v, 8 * i), left)
            right = jnp.where(slot == i, turn(v, 8 * i + 8), right)
        zl[Z_SRC + NY * g : Z_SRC + NY * (g + 1), :] = left
        zr[Z_SRC + NY * g : Z_SRC + NY * (g + 1), :] = right


def extend_z(src, par, co, pown, hl, hr, fl, fr, xl, xr, start, mid, ghost, bricks, cand, pairs):
    first = (lax.axis_index("slab") - 2) * COARSE
    cand[20:24, :] = jnp.zeros((4, 512), F32)
    cand[0:4, :] = fl[0]
    cand[8:12, :] = co[0]
    cand[16:20, :] = fr[0]
    for t in range(4):
        cand[4:8, LANES * t : LANES * (t + 1)] = hl[Z_COARSE + 4 * t : Z_COARSE + 4 * t + 4, :]
        cand[12:16, LANES * t : LANES * (t + 1)] = hr[Z_COARSE + 4 * t : Z_COARSE + 4 * t + 4, :]
    sub, lane = iota((8, LANES), 0), iota((8, LANES), 1)
    chosen = jnp.full((8, LANES), -1, jnp.int32)
    for k in range(4):
        chosen = jnp.where(sub == k + 1, par[0, 0, 2 * k] - first, chosen)
    chosen = chosen.astype(F32)
    chosen = jnp.where(sub == 0, hl[Z_POS : Z_POS + 8, :], chosen)
    chosen = jnp.where(sub == 5, hr[Z_POS : Z_POS + 8, :] + 2.0 * COARSE, chosen)
    pick = onehot(chosen == lane.astype(F32))
    six = dot(pick[:, 0:24], cand[...])
    row2, lane2 = iota((32, LANES), 0), iota((32, LANES), 1)
    spread = onehot(lane2 // 8 == (row2 // 16) * 8 + row2 % 16 // 2)
    c, z = iota((LANES, LANES), 0), iota((LANES, LANES), 1)
    place = onehot(c % 8 == z % 16 // 2)
    zone = iota((32, LANES), 1) // 16
    for t in range(4):
        rows = jnp.concatenate(
            [
                jnp.broadcast_to(six[k : k + 1, LANES * t : LANES * (t + 1)], (32, LANES)) * spread
                for k in range(6)
            ],
            axis=0,
        )
        placed = dot(rows, place)
        total = jnp.zeros((32, LANES), F32)
        for k in range(6):
            total = jnp.where(zone == (7 if k == 0 else k - 1), placed[32 * k : 32 * (k + 1)], total)
        start[32 * t : 32 * (t + 1), :] = total
    bricks[...] = pown[...] + hl[Z_BRICK : Z_BRICK + 32, :] + hr[Z_BRICK : Z_BRICK + 32, :]
    lane32 = iota((NY, LANES), 1)
    for g in range(2):
        left = hl[Z_SRC + NY * g : Z_SRC + NY * (g + 1), :]
        right = hr[Z_SRC + NY * g : Z_SRC + NY * (g + 1), :]
        for i in range(16):
            ghost[16 * g + i] = jnp.where(
                lane32 < 8, turn(right, -8 * i), jnp.where(lane32 >= 120, turn(left, -8 * i - 8), 0.0)
            )
    z2, l2 = iota((2 * LANES, LANES), 0), iota((2 * LANES, LANES), 1)
    join = (z2 < 128) & (z2 // 2 == l2)
    join = join | ((z2 >= 128) & (z2 < 136) & (l2 == 64 + (z2 - 128) // 2))
    join = join | ((z2 >= 248) & (l2 == z2 // 2))
    join = onehot(join)
    for i in range(16):
        for part, ref in ((0, src), (1, ghost)):
            a = ref[2 * i, pl.ds(0, 16, 2), :] + ref[2 * i, pl.ds(1, 16, 2), :]
            b = ref[2 * i + 1, pl.ds(0, 16, 2), :] + ref[2 * i + 1, pl.ds(1, 16, 2), :]
            pairs[16 * i : 16 * (i + 1), LANES * part : LANES * (part + 1)] = a + b
    summed = 0.25 * dot(pairs[...], join)
    for i in range(16):
        mid[i] = summed[16 * i : 16 * (i + 1)]
    for out, rows, m0, f0, b0 in ((xl, 0, 0, 0, 0), (xr, 80, 12, 30, 2)):
        out[X_START : X_START + 48, :] = start[rows : rows + 48, :]
        packed = jnp.zeros((8, LANES), F32)
        for i in range(4):
            out[X_MID + 16 * i : X_MID + 16 * (i + 1), :] = mid[m0 + i]
        for i in range(2):
            out[X_FINE + NY * i : X_FINE + NY * (i + 1), :] = src[f0 + i]
            edge = ghost[f0 + i]
            for y in range(4):
                slot = 4 * i + y
                moved = turn(edge[8 * y : 8 * y + 8], 16 * slot + 8)
                packed = jnp.where(lane // 16 == slot, moved, packed)
        out[X_GHOST : X_GHOST + 8, :] = packed
        out[X_BRICK : X_BRICK + 8, :] = bricks[4 * b0 : 4 * b0 + 8, :]
        out[X_BRICK + 8 : X_BRICK + 16, :] = bricks[16 + 4 * b0 : 24 + 4 * b0, :]


def up_down(v):
    rows = v.shape[0]
    y = iota(v.shape, 0)
    up = jnp.where(y == 0, 0.0, pltpu.roll(v, 1, 0))
    down = jnp.where(y == rows - 1, 0.0, pltpu.roll(v, rows - 1, 0))
    return up + down


def along_y(v, z_sum):
    a = 4.0 * v + z_sum
    b = 4.0 * v + up_down(v)
    c = 4.0 * a + up_down(a)
    return a + b, c


def relax(v, rhs, inverse, weight, before, here, after):
    d = 4.0 * here[0] + (before[0] + after[0])
    e = 4.0 * here[1] + (before[1] + after[1])
    return v + inverse * (rhs - (here[1] + d) * (1.0 / 6.0) - weight * e)


def sweep_all(
    src, xl, xr, start, smid, sghost, bricks, mid_out, fin_out,
    v13, pext, i13, w13, i14, w14, i14g, w14g, m0, g0, m1, g1, fine, fghost,
):
    pext[0:8, :] = xl[X_BRICK : X_BRICK + 8, :]
    pext[8:24, :] = bricks[0:16, :]
    pext[24:32, :] = xr[X_BRICK : X_BRICK + 8, :]
    pext[32:40, :] = xl[X_BRICK + 8 : X_BRICK + 16, :]
    pext[40:56, :] = bricks[16:32, :]
    pext[56:64, :] = xr[X_BRICK + 8 : X_BRICK + 16, :]
    b, l = iota((LANES, 3 * LANES), 0), iota((LANES, 3 * LANES), 1)
    ring = l % LANES
    hit = (l < 128) & (b == jnp.where(ring >= 96, ring // 4 + 96, ring // 4))
    hit = hit | ((l >= 128) & (l < 256) & (b == ring // 8))
    hit = hit | ((l >= 256) & (b == jnp.where(ring >= 64, ring // 8 + 112, ring // 8 + 16)))
    spread = dot(pext[...], onehot(hit))
    factor = relaxation * spread[0:32]
    weight = spread[32:64] * (1.0 / 216.0) - (1.0 / 12.0)
    half = iota((8, LANES), 0) < 4
    for bx in range(8):
        for t in range(2):
            r = 4 * bx + 2 * t
            for table, out in ((factor, i13), (weight, w13)):
                upper = jnp.broadcast_to(table[r : r + 1, 0:LANES], (8, LANES))
                lower = jnp.broadcast_to(table[r + 1 : r + 2, 0:LANES], (8, LANES))
                out[bx, 8 * t : 8 * t + 8, :] = jnp.where(half, upper, lower)
    for bx in range(1, 7):
        for by in range(4):
            r = 4 * bx + by
            for table, out, col in ((factor, i14, 1), (weight, w14, 1), (factor, i14g, 2), (weight, w14g, 2)):
                row = table[r : r + 1, LANES * col : LANES * (col + 1)]
                out[bx - 1, 8 * by : 8 * by + 8, :] = jnp.broadcast_to(row, (8, LANES))

    for x in range(-5, 21):
        q = x // 2
        if q < 0:
            v = xr_rows(xl, X_START + 16 * (q + 3))
        elif q > 7:
            v = xr_rows(xr, X_START + 16 * (q - 8))
        else:
            v = start[16 * q : 16 * (q + 1), :]
        v13[x + 5] = jnp.where(i13[x // 4 + 2] != 0.0, v, 0.0)

    def rhs13(x):
        if x < 0:
            return xl[X_MID + 16 * (x + 4) : X_MID + 16 * (x + 5), :]
        if x > 15:
            return xr[X_MID + 16 * (x - 16) : X_MID + 16 * (x - 15), :]
        return smid[x]

    for n in range(SWEEPS):
        low, high = -4 + n, 19 - n
        planes = {}
        for x in range(low - 1, high + 2):
            v = v13[x + 5]
            planes[x] = along_y(v, turn(v, 1) + turn(v, -1))
            if x > low:
                o = x - 1
                bx = o // 4 + 2
                v13[o + 5] = relax(
                    v13[o + 5], rhs13(o), i13[bx], w13[bx], planes[o - 1], planes[o], planes[o + 1]
                )
    for x in range(16):
        mid_out[x] = v13[x + 5, :, 0:64]

    b, l = iota((LANES, 2 * LANES), 0), iota((LANES, 2 * LANES), 1)
    lift = ((l < 128) & (b == l // 2)) | ((l >= 128) & (l < 192) & (b == l // 2)) | ((l >= 192) & (b == l // 2))
    lift = onehot(lift)
    parents = jnp.concatenate(
        [jnp.where(i13[x // 4 + 2] != 0.0, v13[x + 5], 0.0) for x in range(-2, 18)], axis=0
    )
    lifted = dot(parents, lift)
    for x in range(-2, 18):
        rows = lifted[16 * (x + 2) : 16 * (x + 3)]
        for child in (2 * x, 2 * x + 1):
            if -3 <= child <= 34:
                for parity in range(2):
                    m0[child + 3, pl.ds(parity, 16, 2), :] = rows[:, 0:LANES]
                    g0[child + 3, pl.ds(parity, 16, 2), :] = rows[:, LANES:]
    lane8 = iota((8, LANES), 1)
    valid = (lane8 < 8) | (lane8 >= 120)
    for i in range(2):
        fine[i] = xl[X_FINE + NY * i : X_FINE + NY * (i + 1), :]
        fine[34 + i] = xr[X_FINE + NY * i : X_FINE + NY * (i + 1), :]
        for y in range(4):
            slot = 4 * i + y
            for edge, at in ((xl, i), (xr, 34 + i)):
                moved = turn(edge[X_GHOST : X_GHOST + 8, :], -(16 * slot + 8))
                fghost[at, 8 * y : 8 * y + 8, :] = jnp.where(valid, moved, 0.0)

    lane = iota((NY, LANES), 1)

    def sums(vm, vg, want_main):
        mr, gr, ml, gl = turn(vm, 1), turn(vg, 1), turn(vm, -1), turn(vg, -1)
        if want_main:
            return jnp.where(lane == 0, gr, mr) + jnp.where(lane == 127, gl, ml)
        return jnp.where(lane == 0, mr, gr) + jnp.where(lane == 127, ml, gl)

    def rhs14(x, main):
        if isinstance(x, int) and (x < 0 or x > 31):
            return (fine if main else fghost)[x + 2 if x < 0 else x + 2]
        return (src if main else sghost)[x]

    def sweep14(n, main, vm, vg, out, last):
        low, high = -2 + n, 33 - n
        inv, wgt = (i14, w14) if main else (i14g, w14g)
        own = vm if main else vg

        def plane(x):
            a, g = vm[x + 3], vg[x + 3]
            return along_y(a if main else g, sums(a, g, main))

        def write(x, bx, before, here, after):
            value = relax(own[x + 3], rhs14(x, main), inv[bx], wgt[bx], before, here, after)
            if last:
                out[x] = value
            else:
                out[x + 3] = value

        before, here = plane(low - 1), plane(low)
        for x in range(low, 0):
            after = plane(x + 1)
            write(x, 0, before, here, after)
            before, here = here, after

        def body(step, carry):
            before, here = carry
            for j in range(UNROLL):
                x = step * UNROLL + j
                after = plane(x + 1)
                write(x, (x // 8) + 1 if UNROLL > 8 else step * UNROLL // 8 + 1, before, here, after)
                before, here = here, after
            return before, here

        before, here = lax.fori_loop(0, CX // UNROLL, body, (before, here))
        for x in range(32, high + 1):
            after = plane(x + 1)
            write(x, 5, before, here, after)
            before, here = here, after

    sweep14(0, False, m0, g0, g1, False)
    sweep14(0, True, m0, g0, m1, False)
    sweep14(1, False, m1, g1, g0, False)
    sweep14(1, True, m1, g1, m0, False)
    sweep14(2, True, m0, g0, fin_out, True)


def xr_rows(ref, row):
    return ref[row : row + 16, :]


def build(interpret=False):
    def local(source, occupancy, classes, screen_table, parents, coarse):
        def sds(*shape):
            return jax.ShapeDtypeStruct(shape, F32)

        vm = pl.BlockSpec(memory_space=VMEM)
        sm = pl.BlockSpec(memory_space=SMEM)

        def send(block, axis, step):
            count = lax.axis_size(axis)
            if step > 0:
                pairs = [(i, i + step) for i in range(count - step)]
            else:
                pairs = [(i, i + step) for i in range(-step, count)]
            return lax.ppermute(block, axis, pairs)

        fl = send(coarse, "slab", 2)
        fr = send(coarse, "slab", -2)
        zl, zr, pown = pl.pallas_call(
            pack_z,
            out_shape=(sds(Z_ROWS, LANES), sds(Z_ROWS, LANES), sds(32, LANES)),
            in_specs=[vm, vm, vm, sm, sm, vm],
            out_specs=(vm, vm, vm),
            interpret=interpret,
            compiler_params=pltpu.CompilerParams(vmem_limit_bytes=4 << 20),
            name="pack_z",
        )(source, occupancy, classes, screen_table, parents, coarse)
        hl = send(zr, "slab", 1)
        hr = send(zl, "slab", -1)
        xl, xr, start, mid, ghost, bricks = pl.pallas_call(
            extend_z,
            out_shape=(
                sds(X_ROWS, LANES), sds(X_ROWS, LANES), sds(LANES, LANES), sds(16, 16, LANES),
                sds(CX, NY, LANES), sds(32, LANES),
            ),
            in_specs=[vm, sm] + [vm] * 6,
            out_specs=(vm,) * 6,
            scratch_shapes=[VMEM((24, 512), F32), VMEM((256, 2 * LANES), F32)],
            interpret=interpret,
            compiler_params=pltpu.CompilerParams(vmem_limit_bytes=8 << 20),
            name="extend_z",
        )(source, parents, coarse, pown, hl, hr, fl, fr)
        gl = send(xr, "grp", 1)
        gr = send(xl, "grp", -1)
        return pl.pallas_call(
            sweep_all,
            out_shape=(sds(16, 16, 64), sds(CX, NY, CZ)),
            in_specs=[vm] * 7,
            out_specs=(vm, vm),
            scratch_shapes=[
                VMEM((26, 16, LANES), F32),
                VMEM((64, LANES), F32),
                VMEM((8, 16, LANES), F32),
                VMEM((8, 16, LANES), F32),
            ]
            + [VMEM((6, NY, LANES), F32)] * 4
            + [VMEM((38, NY, LANES), F32)] * 4
            + [VMEM((36, NY, LANES), F32)] * 2,
            interpret=interpret,
            compiler_params=pltpu.CompilerParams(vmem_limit_bytes=16 << 20),
            name="sweep_all",
        )(source, gl, gr, start, mid, ghost, bricks)

    return local


def solution(mesh, interpret=False):
    placed = (
        P("grp", None, "slab"),
        P("grp", None, "slab"),
        P("grp", None, "slab"),
        P(),
        P("grp", None, "slab"),
        P("grp", "slab", None),
    )
    return jax.shard_map(
        build(interpret),
        mesh=mesh,
        in_specs=placed,
        out_specs=(P("grp", None, "slab"), P("grp", None, "slab")),
        check_vma=False,
    )
```

```python
import jax
import jax.numpy as jnp
from jax import lax
from jax.experimental import pallas as pl
from jax.experimental.pallas import tpu as pltpu
from jax.sharding import PartitionSpec as P

BRICK = 8
SWEEPS = 3

screen_strength = 4.0
relaxation = 2.0 / 3.0
stiff_diagonal = 8.0 / 3.0
mass_diagonal = 8.0 / 27.0

F32 = jnp.float32
HI = lax.Precision.HIGHEST
VMEM = pltpu.VMEM
SMEM = pltpu.SMEM

CX, NY, CZ = 32, 32, 128
LANES = 128
COARSE = 4
UNROLL = 8

Z_COARSE, Z_POS, Z_BRICK, Z_SRC, Z_ROWS = 0, 16, 24, 56, 120
X_START, X_MID, X_FINE, X_GHOST, X_BRICK, X_ROWS = 0, 48, 112, 176, 184, 200


def iota(shape, dim):
    return lax.broadcasted_iota(jnp.int32, shape, dim)


def onehot(mask):
    return jnp.where(mask, 1.0, 0.0).astype(F32)


def dot(a, b):
    return jnp.dot(a, b, precision=HI, preferred_element_type=F32)


def turn(v, shift):
    shift = shift % LANES
    return v if shift == 0 else pltpu.roll(v, shift, v.ndim - 1)


def pack_z(
    src_hbm, occ_hbm, cls_hbm, tab_hbm, par_hbm, co_hbm, za, zb, co_out, pown,
    src, occ, cls, tab, par, co, zl, zr, sems,
):
    copies = [
        pltpu.make_async_copy(a, b, sems.at[i])
        for i, (a, b) in enumerate(
            ((occ_hbm, occ), (cls_hbm, cls), (tab_hbm, tab), (par_hbm, par), (co_hbm, co), (src_hbm, src))
        )
    ]
    for copy in copies:
        copy.start()
    slab = lax.axis_index("slab")
    first = (slab - 1) * COARSE
    for copy in copies[:-1]:
        copy.wait()
    for t in range(4):
        part = co[0, :, LANES * t : LANES * (t + 1)]
        zl[Z_COARSE + 4 * t : Z_COARSE + 4 * t + 4, :] = part
        zr[Z_COARSE + 4 * t : Z_COARSE + 4 * t + 4, :] = part
        co_out[4 * t : 4 * t + 4, :] = part
    zl[Z_POS : Z_POS + 8, :] = jnp.full((8, LANES), par[0, 0, 0] - first, jnp.int32).astype(F32)
    zr[Z_POS : Z_POS + 8, :] = jnp.full((8, LANES), par[0, 0, 7] - first, jnp.int32).astype(F32)
    pown[...] = jnp.zeros((32, LANES), F32)
    for bx in range(4):
        occupied = occ[bx].astype(F32)
        labels = cls[bx]
        weight = jnp.zeros((4, 16), F32)
        for c in range(16):
            weight = weight + jnp.where(labels == c, tab[c], 0.0)
        screen = screen_strength * weight
        pown[4 * bx : 4 * bx + 4, 0:16] = occupied / (stiff_diagonal + screen * mass_diagonal)
        pown[16 + 4 * bx : 20 + 4 * bx, 0:16] = screen
    bricks = pown[...]
    lane = iota((32, LANES), 1)
    zl[Z_BRICK : Z_BRICK + 32, :] = jnp.where((lane == 16) | (lane == 17), turn(bricks, 16), 0.0)
    zr[Z_BRICK : Z_BRICK + 32, :] = jnp.where(lane >= 126, turn(bricks, 112), 0.0)
    copies[-1].wait()
    slot = iota((NY, LANES), 1) // 8
    for g in range(2):
        left = jnp.zeros((NY, LANES), F32)
        right = jnp.zeros((NY, LANES), F32)
        for i in range(16):
            v = src[16 * g + i]
            left = jnp.where(slot == i, turn(v, 8 * i), left)
            right = jnp.where(slot == i, turn(v, 8 * i + 8), right)
        zl[Z_SRC + NY * g : Z_SRC + NY * (g + 1), :] = left
        zr[Z_SRC + NY * g : Z_SRC + NY * (g + 1), :] = right
    even = slab % 2 == 0
    za[...] = jnp.where(even, zr[...], zl[...])
    zb[...] = jnp.where(even, zl[...], zr[...])


def extend_z(
    src, par, co, pown, ha, hb, fc, fd, xa, xb, start, mid, ghost, bricks, cand, pairs, hl, hr, xl, xr
):
    slab = lax.axis_index("slab")
    first = (slab - 2) * COARSE
    even = slab % 2 == 0
    hl[...] = jnp.where(even, hb[...], ha[...])
    hr[...] = jnp.where(even, ha[...], hb[...])

    @pl.when(slab == 0)
    def _():
        hl[Z_BRICK : Z_BRICK + 32, :] = jnp.zeros((32, LANES), F32)

    @pl.when(slab == lax.axis_size("slab") - 1)
    def _():
        hr[Z_BRICK : Z_BRICK + 32, :] = jnp.zeros((32, LANES), F32)

    near = slab % 4 < 2
    cand[20:24, :] = jnp.zeros((4, 512), F32)
    cand[8:12, :] = co[0]
    for t in range(4):
        c, d = fc[4 * t : 4 * t + 4, :], fd[4 * t : 4 * t + 4, :]
        cand[0:4, LANES * t : LANES * (t + 1)] = jnp.where(near, d, c)
        cand[16:20, LANES * t : LANES * (t + 1)] = jnp.where(near, c, d)
        cand[4:8, LANES * t : LANES * (t + 1)] = hl[Z_COARSE + 4 * t : Z_COARSE + 4 * t + 4, :]
        cand[12:16, LANES * t : LANES * (t + 1)] = hr[Z_COARSE + 4 * t : Z_COARSE + 4 * t + 4, :]
    sub, lane = iota((8, LANES), 0), iota((8, LANES), 1)
    chosen = jnp.full((8, LANES), -1, jnp.int32)
    for k in range(4):
        chosen = jnp.where(sub == k + 1, par[0, 0, 2 * k] - first, chosen)
    chosen = chosen.astype(F32)
    chosen = jnp.where(sub == 0, hl[Z_POS : Z_POS + 8, :], chosen)
    chosen = jnp.where(sub == 5, hr[Z_POS : Z_POS + 8, :] + 2.0 * COARSE, chosen)
    pick = onehot(chosen == lane.astype(F32))
    six = dot(pick[:, 0:24], cand[...])
    row2, lane2 = iota((32, LANES), 0), iota((32, LANES), 1)
    spread = onehot(lane2 // 8 == (row2 // 16) * 8 + row2 % 16 // 2)
    c, z = iota((LANES, LANES), 0), iota((LANES, LANES), 1)
    place = onehot(c % 8 == z % 16 // 2)
    zone = iota((32, LANES), 1) // 16
    for t in range(4):
        rows = jnp.concatenate(
            [
                jnp.broadcast_to(six[k : k + 1, LANES * t : LANES * (t + 1)], (32, LANES)) * spread
                for k in range(6)
            ],
            axis=0,
        )
        placed = dot(rows, place)
        total = jnp.zeros((32, LANES), F32)
        for k in range(6):
            total = jnp.where(zone == (7 if k == 0 else k - 1), placed[32 * k : 32 * (k + 1)], total)
        start[32 * t : 32 * (t + 1), :] = total
    bricks[...] = pown[...] + hl[Z_BRICK : Z_BRICK + 32, :] + hr[Z_BRICK : Z_BRICK + 32, :]
    lane32 = iota((NY, LANES), 1)
    for g in range(2):
        left = hl[Z_SRC + NY * g : Z_SRC + NY * (g + 1), :]
        right = hr[Z_SRC + NY * g : Z_SRC + NY * (g + 1), :]
        for i in range(16):
            ghost[16 * g + i] = jnp.where(
                lane32 < 8, turn(right, -8 * i), jnp.where(lane32 >= 120, turn(left, -8 * i - 8), 0.0)
            )
    z2, l2 = iota((2 * LANES, LANES), 0), iota((2 * LANES, LANES), 1)
    join = (z2 < 128) & (z2 // 2 == l2)
    join = join | ((z2 >= 128) & (z2 < 136) & (l2 == 64 + (z2 - 128) // 2))
    join = join | ((z2 >= 248) & (l2 == z2 // 2))
    join = onehot(join)
    for i in range(16):
        for part, ref in ((0, src), (1, ghost)):
            a = ref[2 * i, pl.ds(0, 16, 2), :] + ref[2 * i, pl.ds(1, 16, 2), :]
            b = ref[2 * i + 1, pl.ds(0, 16, 2), :] + ref[2 * i + 1, pl.ds(1, 16, 2), :]
            pairs[16 * i : 16 * (i + 1), LANES * part : LANES * (part + 1)] = a + b
    summed = 0.25 * dot(pairs[...], join)
    for i in range(16):
        mid[i] = summed[16 * i : 16 * (i + 1)]
    for out, rows, m0, f0, b0 in ((xl, 0, 0, 0, 0), (xr, 80, 12, 30, 2)):
        out[X_START : X_START + 48, :] = start[rows : rows + 48, :]
        packed = jnp.zeros((8, LANES), F32)
        for i in range(4):
            out[X_MID + 16 * i : X_MID + 16 * (i + 1), :] = mid[m0 + i]
        for i in range(2):
            out[X_FINE + NY * i : X_FINE + NY * (i + 1), :] = src[f0 + i]
            edge = ghost[f0 + i]
            for y in range(4):
                slot = 4 * i + y
                moved = turn(edge[8 * y : 8 * y + 8], 16 * slot + 8)
                packed = jnp.where(lane // 16 == slot, moved, packed)
        out[X_GHOST : X_GHOST + 8, :] = packed
        out[X_BRICK : X_BRICK + 8, :] = bricks[4 * b0 : 4 * b0 + 8, :]
        out[X_BRICK + 8 : X_BRICK + 16, :] = bricks[16 + 4 * b0 : 24 + 4 * b0, :]
    grp_even = lax.axis_index("grp") % 2 == 0
    xa[...] = jnp.where(grp_even, xr[...], xl[...])
    xb[...] = jnp.where(grp_even, xl[...], xr[...])


def up_down(v):
    rows = v.shape[0]
    y = iota(v.shape, 0)
    up = jnp.where(y == 0, 0.0, pltpu.roll(v, 1, 0))
    down = jnp.where(y == rows - 1, 0.0, pltpu.roll(v, rows - 1, 0))
    return up + down


def along_y(v, z_sum):
    a = 4.0 * v + z_sum
    b = 4.0 * v + up_down(v)
    c = 4.0 * a + up_down(a)
    return a + b, c


def relax(v, rhs, inverse, weight, before, here, after):
    d = 4.0 * here[0] + (before[0] + after[0])
    e = 4.0 * here[1] + (before[1] + after[1])
    return v + inverse * (rhs - (here[1] + d) * (1.0 / 6.0) - weight * e)


def sweep_all(
    src, xa, xb, start, smid, sghost, bricks, mid_out, fin_out,
    v13, pext, i13, w13, i14, w14, i14g, w14g, m0, g0, m1, g1, fine, fghost, xl, xr,
):
    grp = lax.axis_index("grp")
    even = grp % 2 == 0
    xl[...] = jnp.where(even, xb[...], xa[...])
    xr[...] = jnp.where(even, xa[...], xb[...])

    @pl.when(grp == 0)
    def _():
        xl[X_BRICK : X_BRICK + 16, :] = jnp.zeros((16, LANES), F32)

    @pl.when(grp == lax.axis_size("grp") - 1)
    def _():
        xr[X_BRICK : X_BRICK + 16, :] = jnp.zeros((16, LANES), F32)

    pext[0:8, :] = xl[X_BRICK : X_BRICK + 8, :]
    pext[8:24, :] = bricks[0:16, :]
    pext[24:32, :] = xr[X_BRICK : X_BRICK + 8, :]
    pext[32:40, :] = xl[X_BRICK + 8 : X_BRICK + 16, :]
    pext[40:56, :] = bricks[16:32, :]
    pext[56:64, :] = xr[X_BRICK + 8 : X_BRICK + 16, :]
    b, l = iota((LANES, 3 * LANES), 0), iota((LANES, 3 * LANES), 1)
    ring = l % LANES
    hit = (l < 128) & (b == jnp.where(ring >= 96, ring // 4 + 96, ring // 4))
    hit = hit | ((l >= 128) & (l < 256) & (b == ring // 8))
    hit = hit | ((l >= 256) & (b == jnp.where(ring >= 64, ring // 8 + 112, ring // 8 + 16)))
    spread = dot(pext[...], onehot(hit))
    factor = relaxation * spread[0:32]
    weight = spread[32:64] * (1.0 / 216.0) - (1.0 / 12.0)
    half = iota((8, LANES), 0) < 4
    for bx in range(8):
        for t in range(2):
            r = 4 * bx + 2 * t
            for table, out in ((factor, i13), (weight, w13)):
                upper = jnp.broadcast_to(table[r : r + 1, 0:LANES], (8, LANES))
                lower = jnp.broadcast_to(table[r + 1 : r + 2, 0:LANES], (8, LANES))
                out[bx, 8 * t : 8 * t + 8, :] = jnp.where(half, upper, lower)
    for bx in range(1, 7):
        for by in range(4):
            r = 4 * bx + by
            for table, out, col in ((factor, i14, 1), (weight, w14, 1), (factor, i14g, 2), (weight, w14g, 2)):
                row = table[r : r + 1, LANES * col : LANES * (col + 1)]
                out[bx - 1, 8 * by : 8 * by + 8, :] = jnp.broadcast_to(row, (8, LANES))

    for x in range(-5, 21):
        q = x // 2
        if q < 0:
            v = xr_rows(xl, X_START + 16 * (q + 3))
        elif q > 7:
            v = xr_rows(xr, X_START + 16 * (q - 8))
        else:
            v = start[16 * q : 16 * (q + 1), :]
        v13[x + 5] = jnp.where(i13[x // 4 + 2] != 0.0, v, 0.0)

    def rhs13(x):
        if x < 0:
            return xl[X_MID + 16 * (x + 4) : X_MID + 16 * (x + 5), :]
        if x > 15:
            return xr[X_MID + 16 * (x - 16) : X_MID + 16 * (x - 15), :]
        return smid[x]

    for n in range(SWEEPS):
        low, high = -4 + n, 19 - n
        planes = {}
        for x in range(low - 1, high + 2):
            v = v13[x + 5]
            planes[x] = along_y(v, turn(v, 1) + turn(v, -1))
            if x > low:
                o = x - 1
                bx = o // 4 + 2
                v13[o + 5] = relax(
                    v13[o + 5], rhs13(o), i13[bx], w13[bx], planes[o - 1], planes[o], planes[o + 1]
                )
    for x in range(16):
        mid_out[x] = v13[x + 5, :, 0:64]

    b, l = iota((LANES, 2 * LANES), 0), iota((LANES, 2 * LANES), 1)
    lift = ((l < 128) & (b == l // 2)) | ((l >= 128) & (l < 192) & (b == l // 2)) | ((l >= 192) & (b == l // 2))
    lift = onehot(lift)
    parents = jnp.concatenate(
        [jnp.where(i13[x // 4 + 2] != 0.0, v13[x + 5], 0.0) for x in range(-2, 18)], axis=0
    )
    lifted = dot(parents, lift)
    for x in range(-2, 18):
        rows = lifted[16 * (x + 2) : 16 * (x + 3)]
        for child in (2 * x, 2 * x + 1):
            if -3 <= child <= 34:
                for parity in range(2):
                    m0[child + 3, pl.ds(parity, 16, 2), :] = rows[:, 0:LANES]
                    g0[child + 3, pl.ds(parity, 16, 2), :] = rows[:, LANES:]
    lane8 = iota((8, LANES), 1)
    valid = (lane8 < 8) | (lane8 >= 120)
    for i in range(2):
        fine[i] = xl[X_FINE + NY * i : X_FINE + NY * (i + 1), :]
        fine[34 + i] = xr[X_FINE + NY * i : X_FINE + NY * (i + 1), :]
        for y in range(4):
            slot = 4 * i + y
            for edge, at in ((xl, i), (xr, 34 + i)):
                moved = turn(edge[X_GHOST : X_GHOST + 8, :], -(16 * slot + 8))
                fghost[at, 8 * y : 8 * y + 8, :] = jnp.where(valid, moved, 0.0)

    lane = iota((NY, LANES), 1)

    def sums(vm, vg, want_main):
        mr, gr, ml, gl = turn(vm, 1), turn(vg, 1), turn(vm, -1), turn(vg, -1)
        if want_main:
            return jnp.where(lane == 0, gr, mr) + jnp.where(lane == 127, gl, ml)
        return jnp.where(lane == 0, mr, gr) + jnp.where(lane == 127, ml, gl)

    def rhs14(x, main):
        if isinstance(x, int) and (x < 0 or x > 31):
            return (fine if main else fghost)[x + 2 if x < 0 else x + 2]
        return (src if main else sghost)[x]

    def sweep14(n, main, vm, vg, out, last):
        low, high = -2 + n, 33 - n
        inv, wgt = (i14, w14) if main else (i14g, w14g)
        own = vm if main else vg

        def plane(x):
            a, g = vm[x + 3], vg[x + 3]
            return along_y(a if main else g, sums(a, g, main))

        def write(x, bx, before, here, after):
            value = relax(own[x + 3], rhs14(x, main), inv[bx], wgt[bx], before, here, after)
            if last:
                out[x] = value
            else:
                out[x + 3] = value

        before, here = plane(low - 1), plane(low)
        for x in range(low, 0):
            after = plane(x + 1)
            write(x, 0, before, here, after)
            before, here = here, after

        def body(step, carry):
            before, here = carry
            for j in range(UNROLL):
                x = step * UNROLL + j
                after = plane(x + 1)
                write(x, (x // 8) + 1 if UNROLL > 8 else step * UNROLL // 8 + 1, before, here, after)
                before, here = here, after
            return before, here

        before, here = lax.fori_loop(0, CX // UNROLL, body, (before, here))
        for x in range(32, high + 1):
            after = plane(x + 1)
            write(x, 5, before, here, after)
            before, here = here, after

    sweep14(0, False, m0, g0, g1, False)
    sweep14(0, True, m0, g0, m1, False)
    sweep14(1, False, m1, g1, g0, False)
    sweep14(1, True, m1, g1, m0, False)
    sweep14(2, True, m0, g0, fin_out, True)


def xr_rows(ref, row):
    return ref[row : row + 16, :]


def pairing(couples):
    partner = {}
    for a, b in couples:
        partner[a], partner[b] = b, a
    return sorted(partner.items())


def pairings(groups, slabs):
    def at(g, s):
        return g * slabs + s

    every = range(groups)
    one = [(at(g, s), at(g, s + 1)) for g in every for s in range(0, slabs, 2)]
    two = [(at(g, s), at(g, s + 1)) for g in every for s in range(1, slabs - 1, 2)]
    two += [(at(g, s), at(g + 1, s)) for g in range(0, groups, 2) for s in (0, slabs - 1)]
    three = [(at(g, s), at(g, s + 2)) for g in every for s in range(slabs) if s % 4 < 2]
    four = [(at(g, s), at(g, s + 2)) for g in every for s in range(slabs - 2) if s % 4 >= 2]
    four += [(at(g, s), at(g, s + 1)) for g in every for s in (0, slabs - 2)]
    five = [(at(g, s), at(g + 1, s)) for g in range(0, groups, 2) for s in range(slabs)]
    six = [(at(g, s), at(g + 1, s)) for g in range(1, groups - 1, 2) for s in range(slabs)]
    six += [(at(g, s), at(g, s + 1)) for g in (0, groups - 1) for s in range(0, slabs, 2)]
    return [pairing(couples) for couples in (one, two, three, four, five, six)]


def build(mesh, interpret=False):
    one, two, three, four, five, six = pairings(mesh.shape["grp"], mesh.shape["slab"])

    def local(source, occupancy, classes, screen_table, parents, coarse):
        def sds(*shape):
            return jax.ShapeDtypeStruct(shape, F32)

        vm = pl.BlockSpec(memory_space=VMEM)
        sm = pl.BlockSpec(memory_space=SMEM)
        hbm = pl.BlockSpec(memory_space=pltpu.HBM)

        def swap(block, pairs):
            return lax.ppermute(block, ("grp", "slab"), pairs)

        za, zb, rows, pown = pl.pallas_call(
            pack_z,
            out_shape=(sds(Z_ROWS, LANES), sds(Z_ROWS, LANES), sds(16, LANES), sds(32, LANES)),
            in_specs=[hbm] * 6,
            out_specs=(vm,) * 4,
            scratch_shapes=[
                VMEM((CX, NY, LANES), F32),
                VMEM((4, 4, 16), jnp.int32),
                VMEM((4, 4, 16), jnp.int32),
                SMEM((16,), F32),
                SMEM((2, 2, 8), jnp.int32),
                VMEM((1, 4, 512), F32),
                VMEM((Z_ROWS, LANES), F32),
                VMEM((Z_ROWS, LANES), F32),
                pltpu.SemaphoreType.DMA((6,)),
            ],
            interpret=interpret,
            compiler_params=pltpu.CompilerParams(vmem_limit_bytes=4 << 20),
            name="pack_z",
        )(*(pltpu.with_memory_space_constraint(x, pltpu.HBM) for x in (source, occupancy, classes, screen_table, parents, coarse)))
        ha = swap(za, one)
        hb = swap(zb, two)
        fc = swap(rows, three)
        fd = swap(rows, four)
        xa, xb, start, mid, ghost, bricks = pl.pallas_call(
            extend_z,
            out_shape=(
                sds(X_ROWS, LANES), sds(X_ROWS, LANES), sds(LANES, LANES), sds(16, 16, LANES),
                sds(CX, NY, LANES), sds(32, LANES),
            ),
            in_specs=[vm, sm] + [vm] * 6,
            out_specs=(vm,) * 6,
            scratch_shapes=[
                VMEM((24, 512), F32),
                VMEM((256, 2 * LANES), F32),
                VMEM((Z_ROWS, LANES), F32),
                VMEM((Z_ROWS, LANES), F32),
                VMEM((X_ROWS, LANES), F32),
                VMEM((X_ROWS, LANES), F32),
            ],
            interpret=interpret,
            compiler_params=pltpu.CompilerParams(vmem_limit_bytes=8 << 20),
            name="extend_z",
        )(source, parents, coarse, pown, ha, hb, fc, fd)
        ga = swap(xa, five)
        gb = swap(xb, six)
        return pl.pallas_call(
            sweep_all,
            out_shape=(sds(16, 16, 64), sds(CX, NY, CZ)),
            in_specs=[vm] * 7,
            out_specs=(vm, vm),
            scratch_shapes=[
                VMEM((26, 16, LANES), F32),
                VMEM((64, LANES), F32),
                VMEM((8, 16, LANES), F32),
                VMEM((8, 16, LANES), F32),
            ]
            + [VMEM((6, NY, LANES), F32)] * 4
            + [VMEM((38, NY, LANES), F32)] * 4
            + [VMEM((36, NY, LANES), F32)] * 2
            + [VMEM((X_ROWS, LANES), F32)] * 2,
            interpret=interpret,
            compiler_params=pltpu.CompilerParams(vmem_limit_bytes=16 << 20),
            name="sweep_all",
        )(source, ga, gb, start, mid, ghost, bricks)

    return local


def solution(mesh, interpret=False):
    placed = (
        P("grp", None, "slab"),
        P("grp", None, "slab"),
        P("grp", None, "slab"),
        P(),
        P("grp", None, "slab"),
        P("grp", "slab", None),
    )
    return jax.shard_map(
        build(mesh, interpret),
        mesh=mesh,
        in_specs=placed,
        out_specs=(P("grp", None, "slab"), P("grp", None, "slab")),
        check_vma=False,
    )
```

```python
import jax
import jax.numpy as jnp
from jax import lax
from jax.experimental import pallas as pl
from jax.experimental.pallas import tpu as pltpu
from jax.sharding import PartitionSpec as P

BRICK = 8
SWEEPS = 3

screen_strength = 4.0
relaxation = 2.0 / 3.0
stiff_diagonal = 8.0 / 3.0
mass_diagonal = 8.0 / 27.0

F32 = jnp.float32
HI = lax.Precision.HIGHEST
VMEM = pltpu.VMEM
SMEM = pltpu.SMEM

CX, NY, CZ = 32, 32, 128
LANES = 128
COARSE = 4

Z_COARSE, Z_POS, Z_BRICK, Z_SRC, Z_ROWS = 0, 16, 24, 32, 96
X_START, X_MID, X_FINE, X_GHOST, X_BRICK, X_ROWS = 0, 24, 88, 152, 160, 168


def iota(shape, dim):
    return lax.broadcasted_iota(jnp.int32, shape, dim)


def onehot(mask):
    return jnp.where(mask, 1.0, 0.0).astype(F32)


def dot(a, b):
    return jnp.dot(a, b, precision=HI, preferred_element_type=F32)


def turn(v, shift):
    shift = shift % LANES
    return v if shift == 0 else pltpu.roll(v, shift, v.ndim - 1)


def y_sum(tiles):
    n = len(tiles)
    sub = iota((8, LANES), 0)
    first = jnp.where(sub == 0, 0.0, pltpu.roll(tiles[n - 1], 1, 0))
    last = jnp.where(sub == 7, 0.0, pltpu.roll(tiles[0], 7, 0))
    up = [first] + tiles[:-1]
    down = tiles[1:] + [last]
    return [a + b for a, b in zip(up, down)]


def along_y(tiles, z_sums):
    four = [4.0 * v for v in tiles]
    a = [v + z for v, z in zip(four, z_sums)]
    b = [v + y for v, y in zip(four, y_sum(tiles))]
    c = [4.0 * v + y for v, y in zip(a, y_sum(a))]
    return [x + y for x, y in zip(a, b)], c


def relax(v, rhs, inverse, weight, d, e, c):
    return v + inverse * ((rhs - (c + d)) - weight * e)


def along_x(before, here, after):
    return 4.0 * here + (before + after)


def pack_z(
    src_hbm, occ_hbm, cls_hbm, tab_hbm, par_hbm, co_hbm, za, zb, co_out, pown, fine,
    src, occ, cls, tab, par, co, zl, zr, sems,
):
    copies = [
        pltpu.make_async_copy(a, b, sems.at[i])
        for i, (a, b) in enumerate(
            ((occ_hbm, occ), (cls_hbm, cls), (tab_hbm, tab), (par_hbm, par), (co_hbm, co), (src_hbm, src))
        )
    ]
    for copy in copies:
        copy.start()
    slab = lax.axis_index("slab")
    first = (slab - 1) * COARSE
    for copy in copies[:-1]:
        copy.wait()
    for t in range(4):
        part = co[0, :, LANES * t : LANES * (t + 1)]
        zl[Z_COARSE + 4 * t : Z_COARSE + 4 * t + 4, :] = part
        co_out[4 * t : 4 * t + 4, :] = part
    zr[Z_COARSE : Z_COARSE + 16, :] = zl[Z_COARSE : Z_COARSE + 16, :]
    zl[Z_POS : Z_POS + 8, :] = jnp.full((8, LANES), par[0, 0, 0] - first, jnp.int32).astype(F32)
    zr[Z_POS : Z_POS + 8, :] = jnp.full((8, LANES), par[0, 0, 7] - first, jnp.int32).astype(F32)
    pown[...] = jnp.zeros((64, LANES), F32)
    for bx in range(4):
        occupied = occ[bx].astype(F32)
        labels = cls[bx]
        weight = jnp.zeros((4, 16), F32)
        for c in range(16):
            weight = weight + jnp.where(labels == c, tab[c], 0.0)
        screen = screen_strength * weight
        inverse = occupied / (stiff_diagonal + screen * mass_diagonal)
        for parity in range(2):
            pown[pl.ds(8 * bx + parity, 4, 2), 0:16] = inverse
            pown[pl.ds(32 + 8 * bx + parity, 4, 2), 0:16] = screen
    lane = iota((8, LANES), 1)
    packed = jnp.zeros((8, LANES), F32)
    for q in range(8):
        packed = jnp.where(lane // 16 == q, turn(pown[8 * q : 8 * q + 8, :], 16 * q), packed)
    zl[Z_BRICK : Z_BRICK + 8, :] = packed
    zr[Z_BRICK : Z_BRICK + 8, :] = packed
    copies[-1].wait()
    slot = lane // 8
    for g in range(2):
        for t in range(4):
            left = jnp.zeros((8, LANES), F32)
            right = jnp.zeros((8, LANES), F32)
            for i in range(16):
                v = 6.0 * src[16 * g + i, pl.ds(t, 8, 4), :]
                fine[16 * g + i, 8 * t : 8 * t + 8, :] = v
                left = jnp.where(slot == i, turn(v, 8 * i), left)
                right = jnp.where(slot == i, turn(v, 8 * i + 8), right)
            row = Z_SRC + 32 * g + 8 * t
            zl[row : row + 8, :] = left
            zr[row : row + 8, :] = right
    even = slab % 2 == 0
    za[...] = jnp.where(even, zr[...], zl[...])
    zb[...] = jnp.where(even, zl[...], zr[...])


def extend_z(
    fine, par, co, pown, ha, hb, fc, fd, xa, xb, start, mid, ghost, bricks, cand, pairs, hl, hr, xl, xr
):
    slab = lax.axis_index("slab")
    first = (slab - 2) * COARSE
    even = slab % 2 == 0
    hl[...] = jnp.where(even, hb[...], ha[...])
    hr[...] = jnp.where(even, ha[...], hb[...])

    @pl.when(slab == 0)
    def _():
        hl[Z_BRICK : Z_BRICK + 8, :] = jnp.zeros((8, LANES), F32)

    @pl.when(slab == lax.axis_size("slab") - 1)
    def _():
        hr[Z_BRICK : Z_BRICK + 8, :] = jnp.zeros((8, LANES), F32)

    near = slab % 4 < 2
    cand[20:24, :] = jnp.zeros((4, 512), F32)
    cand[8:12, :] = co[0]
    for t in range(4):
        c, d = fc[4 * t : 4 * t + 4, :], fd[4 * t : 4 * t + 4, :]
        cand[0:4, LANES * t : LANES * (t + 1)] = jnp.where(near, d, c)
        cand[16:20, LANES * t : LANES * (t + 1)] = jnp.where(near, c, d)
        cand[4:8, LANES * t : LANES * (t + 1)] = hl[Z_COARSE + 4 * t : Z_COARSE + 4 * t + 4, :]
        cand[12:16, LANES * t : LANES * (t + 1)] = hr[Z_COARSE + 4 * t : Z_COARSE + 4 * t + 4, :]
    sub, lane = iota((8, LANES), 0), iota((8, LANES), 1)
    chosen = jnp.full((8, LANES), -1, jnp.int32)
    for k in range(4):
        chosen = jnp.where(sub == k + 1, par[0, 0, 2 * k] - first, chosen)
    chosen = chosen.astype(F32)
    chosen = jnp.where(sub == 0, hl[Z_POS : Z_POS + 8, :], chosen)
    chosen = jnp.where(sub == 5, hr[Z_POS : Z_POS + 8, :] + 2.0 * COARSE, chosen)
    pick = onehot(chosen == lane.astype(F32))
    six = dot(pick[:, 0:24], cand[...])
    row2, lane2 = iota((16, LANES), 0), iota((16, LANES), 1)
    spread = onehot(lane2 // 8 == row2)
    c, z = iota((LANES, LANES), 0), iota((LANES, LANES), 1)
    place = onehot(c % 8 == z % 16 // 2)
    zone = lane2 // 16
    rows = jnp.concatenate(
        [
            jnp.broadcast_to(six[k : k + 1, LANES * t : LANES * (t + 1)], (16, LANES)) * spread
            for t in range(4)
            for k in range(6)
        ],
        axis=0,
    )
    placed = dot(rows, place)
    for t in range(4):
        total = jnp.zeros((16, LANES), F32)
        for k in range(6):
            at = 16 * (6 * t + k)
            total = jnp.where(zone == (7 if k == 0 else k - 1), placed[at : at + 16], total)
        start[16 * t : 16 * (t + 1), :] = total
    for q in range(8):
        low = turn(hl[Z_BRICK : Z_BRICK + 8, :], 112 - 16 * q)
        high = turn(hr[Z_BRICK : Z_BRICK + 8, :], 16 - 16 * q)
        own = pown[8 * q : 8 * q + 8, :]
        bricks[8 * q : 8 * q + 8, :] = jnp.where(lane >= 126, low, jnp.where(lane // 2 == 8, high, own))
    for g in range(2):
        for t in range(4):
            row = Z_SRC + 32 * g + 8 * t
            low, high = turn(hl[row : row + 8, :], -4), turn(hr[row : row + 8, :], 4)
            ghost[32 * g + 8 * t : 32 * g + 8 * t + 8, :] = jnp.where(lane % 8 < 4, low, high)
    z2, l2 = iota((2 * LANES, LANES), 0), iota((2 * LANES, LANES), 1)
    join = (z2 < 128) & (z2 // 2 == l2)
    join = join | ((z2 >= 128) & (z2 < 136) & (l2 == 64 + (z2 - 128) // 2))
    join = join | ((z2 >= 248) & (l2 == z2 // 2))
    join = onehot(join)
    for g in range(2):
        for u in range(2):
            row = Z_SRC + 32 * g + 16 * u
            low = hl[row : row + 8, :] + hl[row + 8 : row + 16, :]
            high = hr[row : row + 8, :] + hr[row + 8 : row + 16, :]
            low, high = low + turn(low, -8), high + turn(high, -8)
            for i in range(8):
                x, at = 2 * (8 * g + i), 16 * (8 * g + i) + 8 * u
                pairs[at : at + 8, 0:LANES] = (
                    fine[x, 16 * u : 16 * u + 8, :]
                    + fine[x, 16 * u + 8 : 16 * u + 16, :]
                    + fine[x + 1, 16 * u : 16 * u + 8, :]
                    + fine[x + 1, 16 * u + 8 : 16 * u + 16, :]
                )
                pairs[at : at + 8, LANES:] = jnp.where(
                    lane < 8, turn(high, -16 * i), jnp.where(lane >= 120, turn(low, 120 - 16 * i), 0.0)
                )
    summed = 0.25 * dot(pairs[...], join)
    for i in range(16):
        mid[i] = summed[16 * i : 16 * (i + 1)]
    for out, rows, m0, f0, g0, b0, edge in ((xl, 0, 0, 0, 0, 0, 0), (xr, 40, 12, 30, 1, 2, 16)):
        out[X_START : X_START + 24, :] = start[rows : rows + 24, :]
        for i in range(4):
            out[X_MID + 16 * i : X_MID + 16 * (i + 1), :] = mid[m0 + i]
        for i in range(2):
            out[X_FINE + NY * i : X_FINE + NY * (i + 1), :] = fine[f0 + i]
        packed = jnp.zeros((8, LANES), F32)
        boxes = jnp.zeros((8, LANES), F32)
        for t in range(4):
            v = ghost[32 * g0 + 8 * t : 32 * g0 + 8 * t + 8, :]
            packed = jnp.where(lane // 16 == t, turn(v, 16 * t + edge), packed)
            at = 32 * (t // 2) + 8 * (b0 + t % 2)
            boxes = jnp.where(lane // 32 == t, turn(bricks[at : at + 8, :], 32 * t + 2), boxes)
        out[X_GHOST : X_GHOST + 8, :] = packed
        out[X_BRICK : X_BRICK + 8, :] = boxes
    grp_even = lax.axis_index("grp") % 2 == 0
    xa[...] = jnp.where(grp_even, xr[...], xl[...])
    xb[...] = jnp.where(grp_even, xl[...], xr[...])


def sweep_all(
    fine, xa, xb, start, smid, sghost, bricks, mid_hbm, fin_hbm,
    v13, pext, coef, rep, m1, m2, xl, xr, mid_out, fin_out, sems,
):
    grp = lax.axis_index("grp")
    even = grp % 2 == 0
    xl[...] = jnp.where(even, xb[...], xa[...])
    xr[...] = jnp.where(even, xa[...], xb[...])

    @pl.when(grp == 0)
    def _():
        xl[X_BRICK : X_BRICK + 8, :] = jnp.zeros((8, LANES), F32)

    @pl.when(grp == lax.axis_size("grp") - 1)
    def _():
        xr[X_BRICK : X_BRICK + 8, :] = jnp.zeros((8, LANES), F32)

    lane = iota((8, LANES), 1)
    ring = (lane < 18) | (lane >= 126)
    for field in range(2):
        pext[64 * field + 16 : 64 * field + 48, :] = bricks[32 * field : 32 * field + 32, :]
        for b in range(2):
            shift = -(32 * (2 * field + b) + 2)
            at = 64 * field + 8 * b
            pext[at : at + 8, :] = jnp.where(ring, turn(xl[X_BRICK : X_BRICK + 8, :], shift), 0.0)
            pext[at + 48 : at + 56, :] = jnp.where(ring, turn(xr[X_BRICK : X_BRICK + 8, :], shift), 0.0)
    b, l = iota((LANES, 3 * LANES), 0), iota((LANES, 3 * LANES), 1)
    z = l % LANES
    hit = (l < 128) & (b == jnp.where(z >= 96, z // 4 + 96, z // 4))
    hit = hit | ((l >= 128) & (l < 256) & (b == z // 8))
    hit = hit | ((l >= 256) & (b == jnp.where(z % 8 < 4, 127, 16)))
    spread = dot(pext[...], onehot(hit))
    coef[0:64, :] = spread[0:64] * (relaxation / 6.0)
    coef[64:128, :] = spread[64:128] * (1.0 / 36.0) - 0.5

    def inverse13(bx):
        return coef[8 * (bx + 2) : 8 * (bx + 3), 0:LANES]

    def weight13(bx):
        return coef[64 + 8 * (bx + 2) : 72 + 8 * (bx + 2), 0:LANES]

    def inverse14(bx):
        return coef[8 * (bx + 2) : 8 * (bx + 3), LANES : 2 * LANES]

    def weight14(bx):
        return coef[64 + 8 * (bx + 2) : 72 + 8 * (bx + 2), LANES : 2 * LANES]

    for x in range(-5, 21):
        q = x // 2
        if q < 0:
            v = xl[X_START + 8 * (q + 3) : X_START + 8 * (q + 4), :]
        elif q > 7:
            v = xr[X_START + 8 * (q - 8) : X_START + 8 * (q - 7), :]
        else:
            v = start[8 * q : 8 * q + 8, :]
        v = jnp.where(inverse13(x // 4) != 0.0, v, 0.0)
        v13[x + 5, 0:8, :] = v
        v13[x + 5, 8:16, :] = v

    def rhs13(x, u):
        if x < 0:
            return xl[X_MID + 16 * (x + 4) + 8 * u : X_MID + 16 * (x + 4) + 8 * u + 8, :]
        if x > 15:
            return xr[X_MID + 16 * (x - 16) + 8 * u : X_MID + 16 * (x - 16) + 8 * u + 8, :]
        return smid[x, 8 * u : 8 * u + 8, :]

    for n in range(SWEEPS):
        low, high = -4 + n, 19 - n
        planes = {}
        for x in range(low - 1, high + 2):
            tiles = [v13[x + 5, 8 * u : 8 * u + 8, :] for u in range(2)]
            planes[x] = along_y(tiles, [turn(v, 1) + turn(v, -1) for v in tiles])
            if x > low:
                o = x - 1
                for u in range(2):
                    d = along_x(planes[o - 1][0][u], planes[o][0][u], planes[x][0][u])
                    e = along_x(planes[o - 1][1][u], planes[o][1][u], planes[x][1][u])
                    v13[o + 5, 8 * u : 8 * u + 8, :] = relax(
                        v13[o + 5, 8 * u : 8 * u + 8, :],
                        rhs13(o, u), inverse13(o // 4), weight13(o // 4), d, e, planes[o][1][u],
                    )
    for x in range(16):
        for u in range(2):
            mid_out[x, pl.ds(u, 8, 2), :] = v13[x + 5, 8 * u : 8 * u + 8, 0:64]
    mid_copy = pltpu.make_async_copy(mid_out, mid_hbm, sems.at[0])
    mid_copy.start()

    b, l = iota((LANES, 2 * LANES), 0), iota((LANES, 2 * LANES), 1)
    j = l % 8
    hit = (l < 128) & (b == l // 2)
    hit = hit | ((l >= 128) & (b == jnp.where(j < 4, 126 + j // 2, 62 + j // 2)))
    parents = jnp.concatenate(
        [
            jnp.where(inverse13(x // 4) != 0.0, v13[x + 5, 8 * u : 8 * u + 8, :], 0.0)
            for x in range(-2, 18)
            for u in range(2)
        ],
        axis=0,
    )
    rep[...] = dot(parents, onehot(hit))

    def parent(q, u):
        return rep[16 * (q + 2) + 8 * u : 16 * (q + 2) + 8 * u + 8, 0:LANES]

    zero = jnp.zeros((8, LANES), F32)
    halo = [[zero, zero] for _ in range(4)]
    for q in range(-2, 18):
        g, i = q // 8 + 1, q % 8
        for u in range(2):
            v = rep[16 * (q + 2) + 8 * u : 16 * (q + 2) + 8 * u + 8, LANES:]
            halo[g][u] = jnp.where(lane // 16 == i, v, halo[g][u])
    halo = [[tiles[t // 2] for t in range(4)] for tiles in halo]
    halo_rhs, halo_inverse, halo_weight = [], [], []
    for g in range(4):
        if g == 0:
            packed = xl[X_GHOST : X_GHOST + 8, :]
            halo_rhs.append([turn(packed, 112 - 16 * t) for t in range(4)])
        elif g == 3:
            packed = xr[X_GHOST : X_GHOST + 8, :]
            halo_rhs.append([turn(packed, -16 * t) for t in range(4)])
        else:
            halo_rhs.append([sghost[32 * (g - 1) + 8 * t : 32 * (g - 1) + 8 * t + 8, :] for t in range(4)])
        for field, out in ((0, halo_inverse), (64, halo_weight)):
            one, two = (coef[field + 8 * (2 * g + k) : field + 8 * (2 * g + k) + 8, 2 * LANES :] for k in range(2))
            out.append(jnp.where(lane < 64, one, two))

    def z_main(v, halo_tile, i):
        edge = turn(halo_tile, -(8 * i + 4))
        return turn(jnp.where(lane == 127, edge, v), 1) + turn(jnp.where(lane == 0, edge, v), -1)

    def sweep_halo(halo, edges):
        planes = []
        for g in range(4):
            right = [jnp.where(lane % 8 == 3, e, v) for e, v in zip(edges[g], halo[g])]
            left = [jnp.where(lane % 8 == 4, e, v) for e, v in zip(edges[g], halo[g])]
            planes.append(along_y(halo[g], [turn(r, 1) + turn(v, -1) for r, v in zip(right, left)]))
        moved = [[[(turn(v, 8), turn(v, -8)) for v in part] for part in plane] for plane in planes]
        out = []
        for g in range(4):
            tiles = []
            for t in range(4):
                de = []
                for part in range(2):
                    before, after = moved[g][part][t]
                    if g > 0:
                        before = jnp.where(lane < 8, moved[g - 1][part][t][0], before)
                    if g < 3:
                        after = jnp.where(lane >= 120, moved[g + 1][part][t][1], after)
                    de.append(along_x(before, planes[g][part][t], after))
                tiles.append(
                    relax(
                        halo[g][t], halo_rhs[g][t], halo_inverse[g], halo_weight[g],
                        de[0], de[1], planes[g][1][t],
                    )
                )
            out.append(tiles)
        return out

    def rhs14(x, t):
        if x < 0:
            return xl[X_FINE + NY * (x + 2) + 8 * t : X_FINE + NY * (x + 2) + 8 * t + 8, :]
        if x > 31:
            return xr[X_FINE + NY * (x - 32) + 8 * t : X_FINE + NY * (x - 32) + 8 * t + 8, :]
        return fine[x, 8 * t : 8 * t + 8, :]

    edges = [[zero, zero] for _ in range(4)]
    for q in range(-2, 18):
        for child in range(2):
            g, i = (2 * q) // 16 + 1, (2 * q) % 16 + child
            for u in range(2):
                edges[g][u] = jnp.where(lane // 8 == i, turn(parent(q, u), 8 * i + 4), edges[g][u])
    edges = [[tiles[t // 2] for t in range(4)] for tiles in edges]
    planes = {}
    for q in range(-2, 18):
        g, i = (2 * q) // 16 + 1, (2 * q) % 16
        tiles = [parent(q, u) for u in range(2)]
        sums = [z_main(tiles[u], halo[g][2 * u], i) for u in range(2)]
        planes[q] = along_y([tiles[t // 2] for t in range(4)], [sums[t // 2] for t in range(4)])
        o = q - 1
        if o >= -1:
            for t in range(4):
                f5, c5 = 5.0 * planes[o][0][t], 5.0 * planes[o][1][t]
                for child in range(2):
                    x, near = 2 * o + child, o - 1 + 2 * child
                    d, e = f5 + planes[near][0][t], c5 + planes[near][1][t]
                    m1[x + 3, 8 * t : 8 * t + 8, :] = relax(
                        parent(o, t // 2), rhs14(x, t), inverse14(x // 8), weight14(x // 8),
                        d, e, planes[o][1][t],
                    )
    halo = sweep_halo(halo, edges)

    pieces = []
    for n, source, target in ((1, m1, m2), (2, m2, None)):
        low, high = -2 + n, 33 - n
        if n == 1:
            edges = [[zero] * 4 for _ in range(4)]
            for x in range(low - 1, high + 2):
                g, i = x // 16 + 1, x % 16
                for t in range(4):
                    v = source[x + 3, 8 * t : 8 * t + 8, :]
                    edges[g][t] = jnp.where(lane // 8 == i, turn(v, 8 * i + 4), edges[g][t])
        planes = {}
        for x in range(low - 1, high + 2):
            g, i = x // 16 + 1, x % 16
            tiles = [source[x + 3, 8 * t : 8 * t + 8, :] for t in range(4)]
            planes[x] = along_y(tiles, [z_main(tiles[t], halo[g][t], i) for t in range(4)])
            if x > low:
                o = x - 1
                for t in range(4):
                    d = along_x(planes[o - 1][0][t], planes[o][0][t], planes[x][0][t])
                    e = along_x(planes[o - 1][1][t], planes[o][1][t], planes[x][1][t])
                    value = relax(
                        source[o + 3, 8 * t : 8 * t + 8, :],
                        rhs14(o, t), inverse14(o // 8), weight14(o // 8), d, e, planes[o][1][t],
                    )
                    if target is None:
                        fin_out[o, pl.ds(t, 8, 4), :] = value
                    else:
                        target[o + 3, 8 * t : 8 * t + 8, :] = value
                if target is None and o % 8 == 7:
                    part = pl.ds(o - 7, 8)
                    pieces.append(pltpu.make_async_copy(fin_out.at[part], fin_hbm.at[part], sems.at[1 + o // 8]))
                    pieces[-1].start()
        if n == 1:
            halo = sweep_halo(halo, edges)
    mid_copy.wait()
    for piece in pieces:
        piece.wait()


def pairing(couples):
    partner = {}
    for a, b in couples:
        partner[a], partner[b] = b, a
    return sorted(partner.items())


def pairings(groups, slabs):
    def at(g, s):
        return g * slabs + s

    every = range(groups)
    one = [(at(g, s), at(g, s + 1)) for g in every for s in range(0, slabs, 2)]
    two = [(at(g, s), at(g, s + 1)) for g in every for s in range(1, slabs - 1, 2)]
    two += [(at(g, s), at(g + 1, s)) for g in range(0, groups, 2) for s in (0, slabs - 1)]
    three = [(at(g, s), at(g, s + 2)) for g in every for s in range(slabs) if s % 4 < 2]
    four = [(at(g, s), at(g, s + 2)) for g in every for s in range(slabs - 2) if s % 4 >= 2]
    four += [(at(g, s), at(g, s + 1)) for g in every for s in (0, slabs - 2)]
    five = [(at(g, s), at(g + 1, s)) for g in range(0, groups, 2) for s in range(slabs)]
    six = [(at(g, s), at(g + 1, s)) for g in range(1, groups - 1, 2) for s in range(slabs)]
    six += [(at(g, s), at(g, s + 1)) for g in (0, groups - 1) for s in range(0, slabs, 2)]
    return [pairing(couples) for couples in (one, two, three, four, five, six)]


def build(mesh, interpret=False):
    one, two, three, four, five, six = pairings(mesh.shape["grp"], mesh.shape["slab"])

    def local(source, occupancy, classes, screen_table, parents, coarse):
        def sds(*shape):
            return jax.ShapeDtypeStruct(shape, F32)

        vm = pl.BlockSpec(memory_space=VMEM)
        sm = pl.BlockSpec(memory_space=SMEM)
        hbm = pl.BlockSpec(memory_space=pltpu.HBM)

        def swap(block, pairs):
            return lax.ppermute(block, ("grp", "slab"), pairs)

        za, zb, rows, pown, fine = pl.pallas_call(
            pack_z,
            out_shape=(
                sds(Z_ROWS, LANES), sds(Z_ROWS, LANES), sds(16, LANES), sds(64, LANES), sds(CX, NY, LANES),
            ),
            in_specs=[hbm] * 6,
            out_specs=(vm,) * 5,
            scratch_shapes=[
                VMEM((CX, NY, LANES), F32),
                VMEM((4, 4, 16), jnp.int32),
                VMEM((4, 4, 16), jnp.int32),
                SMEM((16,), F32),
                SMEM((2, 2, 8), jnp.int32),
                VMEM((1, 4, 512), F32),
                VMEM((Z_ROWS, LANES), F32),
                VMEM((Z_ROWS, LANES), F32),
                pltpu.SemaphoreType.DMA((6,)),
            ],
            interpret=interpret,
            compiler_params=pltpu.CompilerParams(vmem_limit_bytes=4 << 20),
            name="pack_z",
        )(*(pltpu.with_memory_space_constraint(x, pltpu.HBM) for x in (source, occupancy, classes, screen_table, parents, coarse)))
        ha = swap(za, one)
        hb = swap(zb, two)
        fc = swap(rows, three)
        fd = swap(rows, four)
        xa, xb, start, mid, ghost, bricks = pl.pallas_call(
            extend_z,
            out_shape=(
                sds(X_ROWS, LANES), sds(X_ROWS, LANES), sds(64, LANES), sds(16, 16, LANES),
                sds(64, LANES), sds(64, LANES),
            ),
            in_specs=[vm, sm] + [vm] * 6,
            out_specs=(vm,) * 6,
            scratch_shapes=[
                VMEM((24, 512), F32),
                VMEM((256, 2 * LANES), F32),
                VMEM((Z_ROWS, LANES), F32),
                VMEM((Z_ROWS, LANES), F32),
                VMEM((X_ROWS, LANES), F32),
                VMEM((X_ROWS, LANES), F32),
            ],
            interpret=interpret,
            compiler_params=pltpu.CompilerParams(vmem_limit_bytes=8 << 20),
            name="extend_z",
        )(fine, parents, coarse, pown, ha, hb, fc, fd)
        ga = swap(xa, five)
        gb = swap(xb, six)
        return pl.pallas_call(
            sweep_all,
            out_shape=(sds(16, 16, 64), sds(CX, NY, CZ)),
            in_specs=[vm] * 7,
            out_specs=(hbm, hbm),
            scratch_shapes=[
                VMEM((26, 16, LANES), F32),
                VMEM((LANES, LANES), F32),
                VMEM((LANES, 3 * LANES), F32),
                VMEM((320, 2 * LANES), F32),
                VMEM((38, NY, LANES), F32),
                VMEM((38, NY, LANES), F32),
                VMEM((X_ROWS, LANES), F32),
                VMEM((X_ROWS, LANES), F32),
                VMEM((16, 16, 64), F32),
                VMEM((CX, NY, LANES), F32),
                pltpu.SemaphoreType.DMA((5,)),
            ],
            interpret=interpret,
            compiler_params=pltpu.CompilerParams(vmem_limit_bytes=16 << 20),
            name="sweep_all",
        )(fine, ga, gb, start, mid, ghost, bricks)

    return local


def solution(mesh, interpret=False):
    placed = (
        P("grp", None, "slab"),
        P("grp", None, "slab"),
        P("grp", None, "slab"),
        P(),
        P("grp", None, "slab"),
        P("grp", "slab", None),
    )
    return jax.shard_map(
        build(mesh, interpret),
        mesh=mesh,
        in_specs=placed,
        out_specs=(P("grp", None, "slab"), P("grp", None, "slab")),
        check_vma=False,
    )
```

```python
import jax
import jax.numpy as jnp
from jax import lax
from jax.experimental import pallas as pl
from jax.experimental.pallas import tpu as pltpu
from jax.sharding import PartitionSpec as P

BRICK = 8
SWEEPS = 3

screen_strength = 4.0
relaxation = 2.0 / 3.0
stiff_diagonal = 8.0 / 3.0
mass_diagonal = 8.0 / 27.0

F32 = jnp.float32
HI = lax.Precision.HIGHEST
VMEM = pltpu.VMEM
SMEM = pltpu.SMEM

CX, NY, CZ = 32, 32, 128
LANES = 128
COARSE = 4

Z_COARSE, Z_POS, Z_BRICK, Z_SRC, Z_ROWS = 0, 16, 24, 32, 96
X_START, X_MID, X_FINE, X_GHOST, X_BRICK, X_ROWS = 0, 24, 88, 152, 160, 168


def iota(shape, dim):
    return lax.broadcasted_iota(jnp.int32, shape, dim)


def onehot(mask):
    return jnp.where(mask, 1.0, 0.0).astype(F32)


def dot(a, b):
    return jnp.dot(a, b, precision=HI, preferred_element_type=F32)


def turn(v, shift):
    shift = shift % LANES
    return v if shift == 0 else pltpu.roll(v, shift, v.ndim - 1)


def y_sum(tiles):
    n = len(tiles)
    sub = iota((8, LANES), 0)
    first = jnp.where(sub == 0, 0.0, pltpu.roll(tiles[n - 1], 1, 0))
    last = jnp.where(sub == 7, 0.0, pltpu.roll(tiles[0], 7, 0))
    up = [first] + tiles[:-1]
    down = tiles[1:] + [last]
    return [a + b for a, b in zip(up, down)]


def along_y(tiles, z_sums):
    four = [4.0 * v for v in tiles]
    a = [v + z for v, z in zip(four, z_sums)]
    b = [v + y for v, y in zip(four, y_sum(tiles))]
    c = [4.0 * v + y for v, y in zip(a, y_sum(a))]
    return [x + y for x, y in zip(a, b)], c


def relax(v, rhs, inverse, weight, d, e, c):
    return v + inverse * ((rhs - (c + d)) - weight * e)


def along_x(before, here, after):
    return 4.0 * here + (before + after)


def pack_z(
    src_hbm, occ_hbm, cls_hbm, tab_hbm, par_hbm, co_hbm, za, zb, co_out, pown, fine,
    src, occ, cls, tab, par, co, zl, zr, sems,
):
    copies = [
        pltpu.make_async_copy(a, b, sems.at[i])
        for i, (a, b) in enumerate(
            ((occ_hbm, occ), (cls_hbm, cls), (tab_hbm, tab), (par_hbm, par), (co_hbm, co), (src_hbm, src))
        )
    ]
    for copy in copies:
        copy.start()
    slab = lax.axis_index("slab")
    first = (slab - 1) * COARSE
    for copy in copies[:-1]:
        copy.wait()
    for t in range(4):
        part = co[0, :, LANES * t : LANES * (t + 1)]
        zl[Z_COARSE + 4 * t : Z_COARSE + 4 * t + 4, :] = part
        co_out[4 * t : 4 * t + 4, :] = part
    zr[Z_COARSE : Z_COARSE + 16, :] = zl[Z_COARSE : Z_COARSE + 16, :]
    zl[Z_POS : Z_POS + 8, :] = jnp.full((8, LANES), par[0, 0, 0] - first, jnp.int32).astype(F32)
    zr[Z_POS : Z_POS + 8, :] = jnp.full((8, LANES), par[0, 0, 7] - first, jnp.int32).astype(F32)
    pown[...] = jnp.zeros((64, LANES), F32)
    for bx in range(4):
        occupied = occ[bx].astype(F32)
        labels = cls[bx]
        weight = jnp.zeros((4, 16), F32)
        for c in range(16):
            weight = weight + jnp.where(labels == c, tab[c], 0.0)
        screen = screen_strength * weight
        inverse = occupied / (stiff_diagonal + screen * mass_diagonal)
        for parity in range(2):
            pown[pl.ds(8 * bx + parity, 4, 2), 0:16] = inverse
            pown[pl.ds(32 + 8 * bx + parity, 4, 2), 0:16] = screen
    lane = iota((8, LANES), 1)
    packed = jnp.zeros((8, LANES), F32)
    for q in range(8):
        packed = jnp.where(lane // 16 == q, turn(pown[8 * q : 8 * q + 8, :], 16 * q), packed)
    zl[Z_BRICK : Z_BRICK + 8, :] = packed
    zr[Z_BRICK : Z_BRICK + 8, :] = packed
    copies[-1].wait()
    slot = lane // 8
    for g in range(2):
        for t in range(4):
            left = jnp.zeros((8, LANES), F32)
            right = jnp.zeros((8, LANES), F32)
            for i in range(16):
                v = 6.0 * src[16 * g + i, pl.ds(t, 8, 4), :]
                fine[16 * g + i, 8 * t : 8 * t + 8, :] = v
                left = jnp.where(slot == i, turn(v, 8 * i), left)
                right = jnp.where(slot == i, turn(v, 8 * i + 8), right)
            row = Z_SRC + 32 * g + 8 * t
            zl[row : row + 8, :] = left
            zr[row : row + 8, :] = right
    even = slab % 2 == 0
    za[...] = jnp.where(even, zr[...], zl[...])
    zb[...] = jnp.where(even, zl[...], zr[...])


def extend_z(
    fine, par, co, pown, ha, hb, fc, fd, xa, xb, start, mid, ghost, bricks, cand, pairs, hl, hr, xl, xr
):
    slab = lax.axis_index("slab")
    first = (slab - 2) * COARSE
    even = slab % 2 == 0
    hl[...] = jnp.where(even, hb[...], ha[...])
    hr[...] = jnp.where(even, ha[...], hb[...])

    @pl.when(slab == 0)
    def _():
        hl[Z_BRICK : Z_BRICK + 8, :] = jnp.zeros((8, LANES), F32)

    @pl.when(slab == lax.axis_size("slab") - 1)
    def _():
        hr[Z_BRICK : Z_BRICK + 8, :] = jnp.zeros((8, LANES), F32)

    near = slab % 4 < 2
    cand[20:24, :] = jnp.zeros((4, 512), F32)
    cand[8:12, :] = co[0]
    for t in range(4):
        c, d = fc[4 * t : 4 * t + 4, :], fd[4 * t : 4 * t + 4, :]
        cand[0:4, LANES * t : LANES * (t + 1)] = jnp.where(near, d, c)
        cand[16:20, LANES * t : LANES * (t + 1)] = jnp.where(near, c, d)
        cand[4:8, LANES * t : LANES * (t + 1)] = hl[Z_COARSE + 4 * t : Z_COARSE + 4 * t + 4, :]
        cand[12:16, LANES * t : LANES * (t + 1)] = hr[Z_COARSE + 4 * t : Z_COARSE + 4 * t + 4, :]
    sub, lane = iota((8, LANES), 0), iota((8, LANES), 1)
    chosen = jnp.full((8, LANES), -1, jnp.int32)
    for k in range(4):
        chosen = jnp.where(sub == k + 1, par[0, 0, 2 * k] - first, chosen)
    chosen = chosen.astype(F32)
    chosen = jnp.where(sub == 0, hl[Z_POS : Z_POS + 8, :], chosen)
    chosen = jnp.where(sub == 5, hr[Z_POS : Z_POS + 8, :] + 2.0 * COARSE, chosen)
    pick = onehot(chosen == lane.astype(F32))
    six = dot(pick[:, 0:24], cand[...])
    row2, lane2 = iota((16, LANES), 0), iota((16, LANES), 1)
    spread = onehot(lane2 // 8 == row2)
    c, z = iota((LANES, LANES), 0), iota((LANES, LANES), 1)
    place = onehot(c % 8 == z % 16 // 2)
    zone = lane2 // 16
    rows = jnp.concatenate(
        [
            jnp.broadcast_to(six[k : k + 1, LANES * t : LANES * (t + 1)], (16, LANES)) * spread
            for t in range(4)
            for k in range(6)
        ],
        axis=0,
    )
    placed = dot(rows, place)
    for t in range(4):
        total = jnp.zeros((16, LANES), F32)
        for k in range(6):
            at = 16 * (6 * t + k)
            total = jnp.where(zone == (7 if k == 0 else k - 1), placed[at : at + 16], total)
        start[16 * t : 16 * (t + 1), :] = total
    for q in range(8):
        low = turn(hl[Z_BRICK : Z_BRICK + 8, :], 112 - 16 * q)
        high = turn(hr[Z_BRICK : Z_BRICK + 8, :], 16 - 16 * q)
        own = pown[8 * q : 8 * q + 8, :]
        bricks[8 * q : 8 * q + 8, :] = jnp.where(lane >= 126, low, jnp.where(lane // 2 == 8, high, own))
    for g in range(2):
        for t in range(4):
            row = Z_SRC + 32 * g + 8 * t
            low, high = turn(hl[row : row + 8, :], -4), turn(hr[row : row + 8, :], 4)
            ghost[32 * g + 8 * t : 32 * g + 8 * t + 8, :] = jnp.where(lane % 8 < 4, low, high)
    z2, l2 = iota((2 * LANES, LANES), 0), iota((2 * LANES, LANES), 1)
    join = (z2 < 128) & (z2 // 2 == l2)
    join = join | ((z2 >= 128) & (z2 < 136) & (l2 == 64 + (z2 - 128) // 2))
    join = join | ((z2 >= 248) & (l2 == z2 // 2))
    join = onehot(join)
    for g in range(2):
        for u in range(2):
            row = Z_SRC + 32 * g + 16 * u
            low = hl[row : row + 8, :] + hl[row + 8 : row + 16, :]
            high = hr[row : row + 8, :] + hr[row + 8 : row + 16, :]
            low, high = low + turn(low, -8), high + turn(high, -8)
            for i in range(8):
                x, at = 2 * (8 * g + i), 16 * (8 * g + i) + 8 * u
                pairs[at : at + 8, 0:LANES] = (
                    fine[x, 16 * u : 16 * u + 8, :]
                    + fine[x, 16 * u + 8 : 16 * u + 16, :]
                    + fine[x + 1, 16 * u : 16 * u + 8, :]
                    + fine[x + 1, 16 * u + 8 : 16 * u + 16, :]
                )
                pairs[at : at + 8, LANES:] = jnp.where(
                    lane < 8, turn(high, -16 * i), jnp.where(lane >= 120, turn(low, 120 - 16 * i), 0.0)
                )
    summed = 0.25 * dot(pairs[...], join)
    for i in range(16):
        mid[i] = summed[16 * i : 16 * (i + 1)]
    for out, rows, m0, f0, g0, b0, edge in ((xl, 0, 0, 0, 0, 0, 0), (xr, 40, 12, 30, 1, 2, 16)):
        out[X_START : X_START + 24, :] = start[rows : rows + 24, :]
        for i in range(4):
            out[X_MID + 16 * i : X_MID + 16 * (i + 1), :] = mid[m0 + i]
        for i in range(2):
            out[X_FINE + NY * i : X_FINE + NY * (i + 1), :] = fine[f0 + i]
        packed = jnp.zeros((8, LANES), F32)
        boxes = jnp.zeros((8, LANES), F32)
        for t in range(4):
            v = ghost[32 * g0 + 8 * t : 32 * g0 + 8 * t + 8, :]
            packed = jnp.where(lane // 16 == t, turn(v, 16 * t + edge), packed)
            at = 32 * (t // 2) + 8 * (b0 + t % 2)
            boxes = jnp.where(lane // 32 == t, turn(bricks[at : at + 8, :], 32 * t + 2), boxes)
        out[X_GHOST : X_GHOST + 8, :] = packed
        out[X_BRICK : X_BRICK + 8, :] = boxes
    grp_even = lax.axis_index("grp") % 2 == 0
    xa[...] = jnp.where(grp_even, xr[...], xl[...])
    xb[...] = jnp.where(grp_even, xl[...], xr[...])


def sweep_all(
    fine, xa, xb, start, smid, sghost, bricks, mid_hbm, fin_hbm,
    v13, pext, coef, rep, m1, m2, xl, xr, mid_out, fin_out, sems,
):
    grp = lax.axis_index("grp")
    even = grp % 2 == 0
    xl[...] = jnp.where(even, xb[...], xa[...])
    xr[...] = jnp.where(even, xa[...], xb[...])

    @pl.when(grp == 0)
    def _():
        xl[X_BRICK : X_BRICK + 8, :] = jnp.zeros((8, LANES), F32)

    @pl.when(grp == lax.axis_size("grp") - 1)
    def _():
        xr[X_BRICK : X_BRICK + 8, :] = jnp.zeros((8, LANES), F32)

    lane = iota((8, LANES), 1)
    ring = (lane < 18) | (lane >= 126)
    for field in range(2):
        pext[64 * field + 16 : 64 * field + 48, :] = bricks[32 * field : 32 * field + 32, :]
        for b in range(2):
            shift = -(32 * (2 * field + b) + 2)
            at = 64 * field + 8 * b
            pext[at : at + 8, :] = jnp.where(ring, turn(xl[X_BRICK : X_BRICK + 8, :], shift), 0.0)
            pext[at + 48 : at + 56, :] = jnp.where(ring, turn(xr[X_BRICK : X_BRICK + 8, :], shift), 0.0)
    b, l = iota((LANES, 3 * LANES), 0), iota((LANES, 3 * LANES), 1)
    z = l % LANES
    hit = (l < 128) & (b == jnp.where(z >= 96, z // 4 + 96, z // 4))
    hit = hit | ((l >= 128) & (l < 256) & (b == z // 8))
    hit = hit | ((l >= 256) & (b == jnp.where(z % 8 < 4, 127, 16)))
    spread = dot(pext[...], onehot(hit))
    coef[0:64, :] = spread[0:64] * (relaxation / 6.0)
    coef[64:128, :] = spread[64:128] * (1.0 / 36.0) - 0.5

    def inverse13(bx):
        return coef[8 * (bx + 2) : 8 * (bx + 3), 0:LANES]

    def weight13(bx):
        return coef[64 + 8 * (bx + 2) : 72 + 8 * (bx + 2), 0:LANES]

    def inverse14(bx):
        return coef[8 * (bx + 2) : 8 * (bx + 3), LANES : 2 * LANES]

    def weight14(bx):
        return coef[64 + 8 * (bx + 2) : 72 + 8 * (bx + 2), LANES : 2 * LANES]

    for x in range(-5, 21):
        q = x // 2
        if q < 0:
            v = xl[X_START + 8 * (q + 3) : X_START + 8 * (q + 4), :]
        elif q > 7:
            v = xr[X_START + 8 * (q - 8) : X_START + 8 * (q - 7), :]
        else:
            v = start[8 * q : 8 * q + 8, :]
        v = jnp.where(inverse13(x // 4) != 0.0, v, 0.0)
        v13[x + 5, 0:8, :] = v
        v13[x + 5, 8:16, :] = v

    def rhs13(x, u):
        if x < 0:
            return xl[X_MID + 16 * (x + 4) + 8 * u : X_MID + 16 * (x + 4) + 8 * u + 8, :]
        if x > 15:
            return xr[X_MID + 16 * (x - 16) + 8 * u : X_MID + 16 * (x - 16) + 8 * u + 8, :]
        return smid[x, 8 * u : 8 * u + 8, :]

    for n in range(SWEEPS):
        low, high = -4 + n, 19 - n
        planes = {}
        for x in range(low - 1, high + 2):
            tiles = [v13[x + 5, 8 * u : 8 * u + 8, :] for u in range(2)]
            planes[x] = along_y(tiles, [turn(v, 1) + turn(v, -1) for v in tiles])
            if x > low:
                o = x - 1
                for u in range(2):
                    d = along_x(planes[o - 1][0][u], planes[o][0][u], planes[x][0][u])
                    e = along_x(planes[o - 1][1][u], planes[o][1][u], planes[x][1][u])
                    v13[o + 5, 8 * u : 8 * u + 8, :] = relax(
                        v13[o + 5, 8 * u : 8 * u + 8, :],
                        rhs13(o, u), inverse13(o // 4), weight13(o // 4), d, e, planes[o][1][u],
                    )
    for x in range(16):
        for u in range(2):
            mid_out[x, pl.ds(u, 8, 2), :] = v13[x + 5, 8 * u : 8 * u + 8, 0:64]
    mid_copy = pltpu.make_async_copy(mid_out, mid_hbm, sems.at[0])
    mid_copy.start()

    b, l = iota((LANES, 2 * LANES), 0), iota((LANES, 2 * LANES), 1)
    j = l % 8
    hit = (l < 128) & (b == l // 2)
    hit = hit | ((l >= 128) & (b == jnp.where(j < 4, 126 + j // 2, 62 + j // 2)))
    parents = jnp.concatenate(
        [
            jnp.where(inverse13(x // 4) != 0.0, v13[x + 5, 8 * u : 8 * u + 8, :], 0.0)
            for x in range(-2, 18)
            for u in range(2)
        ],
        axis=0,
    )
    rep[...] = dot(parents, onehot(hit))

    def parent(q, u):
        return rep[16 * (q + 2) + 8 * u : 16 * (q + 2) + 8 * u + 8, 0:LANES]

    zero = jnp.zeros((8, LANES), F32)
    halo = [[zero, zero] for _ in range(4)]
    for q in range(-2, 18):
        g, i = q // 8 + 1, q % 8
        for u in range(2):
            v = rep[16 * (q + 2) + 8 * u : 16 * (q + 2) + 8 * u + 8, LANES:]
            halo[g][u] = jnp.where(lane // 16 == i, v, halo[g][u])
    halo = [[tiles[t // 2] for t in range(4)] for tiles in halo]
    halo_rhs, halo_inverse, halo_weight = [], [], []
    for g in range(4):
        if g == 0:
            packed = xl[X_GHOST : X_GHOST + 8, :]
            halo_rhs.append([turn(packed, 112 - 16 * t) for t in range(4)])
        elif g == 3:
            packed = xr[X_GHOST : X_GHOST + 8, :]
            halo_rhs.append([turn(packed, -16 * t) for t in range(4)])
        else:
            halo_rhs.append([sghost[32 * (g - 1) + 8 * t : 32 * (g - 1) + 8 * t + 8, :] for t in range(4)])
        for field, out in ((0, halo_inverse), (64, halo_weight)):
            one, two = (coef[field + 8 * (2 * g + k) : field + 8 * (2 * g + k) + 8, 2 * LANES :] for k in range(2))
            out.append(jnp.where(lane < 64, one, two))

    def z_main(v, halo_tile, i):
        edge = turn(halo_tile, -(8 * i + 4))
        return turn(jnp.where(lane == 127, edge, v), 1) + turn(jnp.where(lane == 0, edge, v), -1)

    def sweep_halo(halo, edges):
        planes = []
        for g in range(4):
            right = [jnp.where(lane % 8 == 3, e, v) for e, v in zip(edges[g], halo[g])]
            left = [jnp.where(lane % 8 == 4, e, v) for e, v in zip(edges[g], halo[g])]
            planes.append(along_y(halo[g], [turn(r, 1) + turn(v, -1) for r, v in zip(right, left)]))
        moved = [[[(turn(v, 8), turn(v, -8)) for v in part] for part in plane] for plane in planes]
        out = []
        for g in range(4):
            tiles = []
            for t in range(4):
                de = []
                for part in range(2):
                    before, after = moved[g][part][t]
                    if g > 0:
                        before = jnp.where(lane < 8, moved[g - 1][part][t][0], before)
                    if g < 3:
                        after = jnp.where(lane >= 120, moved[g + 1][part][t][1], after)
                    de.append(along_x(before, planes[g][part][t], after))
                tiles.append(
                    relax(
                        halo[g][t], halo_rhs[g][t], halo_inverse[g], halo_weight[g],
                        de[0], de[1], planes[g][1][t],
                    )
                )
            out.append(tiles)
        return out

    def rhs14(x, t):
        if x < 0:
            return xl[X_FINE + NY * (x + 2) + 8 * t : X_FINE + NY * (x + 2) + 8 * t + 8, :]
        if x > 31:
            return xr[X_FINE + NY * (x - 32) + 8 * t : X_FINE + NY * (x - 32) + 8 * t + 8, :]
        return fine[x, 8 * t : 8 * t + 8, :]

    edges = [[zero, zero] for _ in range(4)]
    for q in range(-2, 18):
        for child in range(2):
            g, i = (2 * q) // 16 + 1, (2 * q) % 16 + child
            for u in range(2):
                edges[g][u] = jnp.where(lane // 8 == i, turn(parent(q, u), 8 * i + 4), edges[g][u])
    edges = [[tiles[t // 2] for t in range(4)] for tiles in edges]
    planes = {}
    for q in range(-2, 18):
        g, i = (2 * q) // 16 + 1, (2 * q) % 16
        tiles = [parent(q, u) for u in range(2)]
        sums = [z_main(tiles[u], halo[g][2 * u], i) for u in range(2)]
        planes[q] = along_y([tiles[t // 2] for t in range(4)], [sums[t // 2] for t in range(4)])
        o = q - 1
        if o >= -1:
            for t in range(4):
                f5, c5 = 5.0 * planes[o][0][t], 5.0 * planes[o][1][t]
                for child in range(2):
                    x, near = 2 * o + child, o - 1 + 2 * child
                    d, e = f5 + planes[near][0][t], c5 + planes[near][1][t]
                    m1[x + 3, 8 * t : 8 * t + 8, :] = relax(
                        parent(o, t // 2), rhs14(x, t), inverse14(x // 8), weight14(x // 8),
                        d, e, planes[o][1][t],
                    )
    halo = sweep_halo(halo, edges)

    pieces = []
    for n, source, target in ((1, m1, m2), (2, m2, None)):
        low, high = -2 + n, 33 - n
        if n == 1:
            edges = [[zero] * 4 for _ in range(4)]
            b, l = iota((LANES, LANES), 0), iota((LANES, LANES), 1)
            hit = ((b == 127) & (l % 8 == 3)) | ((b == 0) & (l % 8 == 4))
            wide = [source[x + 3] for x in range(low - 1, high + 2)]
            wide = dot(jnp.concatenate(wide, axis=0), onehot(hit))
            for x in range(low - 1, high + 2):
                g, i = x // 16 + 1, x % 16
                for t in range(4):
                    at = 32 * (x - low + 1) + 8 * t
                    edges[g][t] = jnp.where(lane // 8 == i, wide[at : at + 8], edges[g][t])
        planes = {}
        for x in range(low - 1, high + 2):
            g, i = x // 16 + 1, x % 16
            tiles = [source[x + 3, 8 * t : 8 * t + 8, :] for t in range(4)]
            planes[x] = along_y(tiles, [z_main(tiles[t], halo[g][t], i) for t in range(4)])
            if x > low:
                o = x - 1
                for t in range(4):
                    d = along_x(planes[o - 1][0][t], planes[o][0][t], planes[x][0][t])
                    e = along_x(planes[o - 1][1][t], planes[o][1][t], planes[x][1][t])
                    value = relax(
                        source[o + 3, 8 * t : 8 * t + 8, :],
                        rhs14(o, t), inverse14(o // 8), weight14(o // 8), d, e, planes[o][1][t],
                    )
                    if target is None:
                        fin_out[o, pl.ds(t, 8, 4), :] = value
                    else:
                        target[o + 3, 8 * t : 8 * t + 8, :] = value
                if target is None and o % 8 == 7:
                    part = pl.ds(o - 7, 8)
                    pieces.append(pltpu.make_async_copy(fin_out.at[part], fin_hbm.at[part], sems.at[1 + o // 8]))
                    pieces[-1].start()
        if n == 1:
            halo = sweep_halo(halo, edges)
    mid_copy.wait()
    for piece in pieces:
        piece.wait()


def pairing(couples):
    partner = {}
    for a, b in couples:
        partner[a], partner[b] = b, a
    return sorted(partner.items())


def pairings(groups, slabs):
    def at(g, s):
        return g * slabs + s

    every = range(groups)
    one = [(at(g, s), at(g, s + 1)) for g in every for s in range(0, slabs, 2)]
    two = [(at(g, s), at(g, s + 1)) for g in every for s in range(1, slabs - 1, 2)]
    two += [(at(g, s), at(g + 1, s)) for g in range(0, groups, 2) for s in (0, slabs - 1)]
    three = [(at(g, s), at(g, s + 2)) for g in every for s in range(slabs) if s % 4 < 2]
    four = [(at(g, s), at(g, s + 2)) for g in every for s in range(slabs - 2) if s % 4 >= 2]
    four += [(at(g, s), at(g, s + 1)) for g in every for s in (0, slabs - 2)]
    five = [(at(g, s), at(g + 1, s)) for g in range(0, groups, 2) for s in range(slabs)]
    six = [(at(g, s), at(g + 1, s)) for g in range(1, groups - 1, 2) for s in range(slabs)]
    six += [(at(g, s), at(g, s + 1)) for g in (0, groups - 1) for s in range(0, slabs, 2)]
    return [pairing(couples) for couples in (one, two, three, four, five, six)]


def build(mesh, interpret=False):
    one, two, three, four, five, six = pairings(mesh.shape["grp"], mesh.shape["slab"])

    def local(source, occupancy, classes, screen_table, parents, coarse):
        def sds(*shape):
            return jax.ShapeDtypeStruct(shape, F32)

        vm = pl.BlockSpec(memory_space=VMEM)
        sm = pl.BlockSpec(memory_space=SMEM)
        hbm = pl.BlockSpec(memory_space=pltpu.HBM)

        def swap(block, pairs):
            return lax.ppermute(block, ("grp", "slab"), pairs)

        za, zb, rows, pown, fine = pl.pallas_call(
            pack_z,
            out_shape=(
                sds(Z_ROWS, LANES), sds(Z_ROWS, LANES), sds(16, LANES), sds(64, LANES), sds(CX, NY, LANES),
            ),
            in_specs=[hbm] * 6,
            out_specs=(vm,) * 5,
            scratch_shapes=[
                VMEM((CX, NY, LANES), F32),
                VMEM((4, 4, 16), jnp.int32),
                VMEM((4, 4, 16), jnp.int32),
                SMEM((16,), F32),
                SMEM((2, 2, 8), jnp.int32),
                VMEM((1, 4, 512), F32),
                VMEM((Z_ROWS, LANES), F32),
                VMEM((Z_ROWS, LANES), F32),
                pltpu.SemaphoreType.DMA((6,)),
            ],
            interpret=interpret,
            compiler_params=pltpu.CompilerParams(vmem_limit_bytes=4 << 20),
            name="pack_z",
        )(*(pltpu.with_memory_space_constraint(x, pltpu.HBM) for x in (source, occupancy, classes, screen_table, parents, coarse)))
        ha = swap(za, one)
        hb = swap(zb, two)
        fc = swap(rows, three)
        fd = swap(rows, four)
        xa, xb, start, mid, ghost, bricks = pl.pallas_call(
            extend_z,
            out_shape=(
                sds(X_ROWS, LANES), sds(X_ROWS, LANES), sds(64, LANES), sds(16, 16, LANES),
                sds(64, LANES), sds(64, LANES),
            ),
            in_specs=[vm, sm] + [vm] * 6,
            out_specs=(vm,) * 6,
            scratch_shapes=[
                VMEM((24, 512), F32),
                VMEM((256, 2 * LANES), F32),
                VMEM((Z_ROWS, LANES), F32),
                VMEM((Z_ROWS, LANES), F32),
                VMEM((X_ROWS, LANES), F32),
                VMEM((X_ROWS, LANES), F32),
            ],
            interpret=interpret,
            compiler_params=pltpu.CompilerParams(vmem_limit_bytes=8 << 20),
            name="extend_z",
        )(fine, parents, coarse, pown, ha, hb, fc, fd)
        ga = swap(xa, five)
        gb = swap(xb, six)
        return pl.pallas_call(
            sweep_all,
            out_shape=(sds(16, 16, 64), sds(CX, NY, CZ)),
            in_specs=[vm] * 7,
            out_specs=(hbm, hbm),
            scratch_shapes=[
                VMEM((26, 16, LANES), F32),
                VMEM((LANES, LANES), F32),
                VMEM((LANES, 3 * LANES), F32),
                VMEM((320, 2 * LANES), F32),
                VMEM((38, NY, LANES), F32),
                VMEM((38, NY, LANES), F32),
                VMEM((X_ROWS, LANES), F32),
                VMEM((X_ROWS, LANES), F32),
                VMEM((16, 16, 64), F32),
                VMEM((CX, NY, LANES), F32),
                pltpu.SemaphoreType.DMA((5,)),
            ],
            interpret=interpret,
            compiler_params=pltpu.CompilerParams(vmem_limit_bytes=16 << 20),
            name="sweep_all",
        )(fine, ga, gb, start, mid, ghost, bricks)

    return local


def solution(mesh, interpret=False):
    placed = (
        P("grp", None, "slab"),
        P("grp", None, "slab"),
        P("grp", None, "slab"),
        P(),
        P("grp", None, "slab"),
        P("grp", "slab", None),
    )
    return jax.shard_map(
        build(mesh, interpret),
        mesh=mesh,
        in_specs=placed,
        out_specs=(P("grp", None, "slab"), P("grp", None, "slab")),
        check_vma=False,
    )
```

```python
import jax
import jax.numpy as jnp
from jax import lax
from jax.experimental import pallas as pl
from jax.experimental.pallas import tpu as pltpu
from jax.sharding import PartitionSpec as P

SWEEPS = 3

screen_strength = 4.0
relaxation = 2.0 / 3.0
stiff_diagonal = 8.0 / 3.0
mass_diagonal = 8.0 / 27.0

F32 = jnp.float32
HI = lax.Precision.HIGHEST
VMEM = pltpu.VMEM
SMEM = pltpu.SMEM

CX, NY, CZ = 32, 32, 128
LANES = 128
COARSE = 4

Z_COARSE, Z_POS, Z_BRICK, Z_SRC, Z_ROWS = 0, 16, 24, 32, 96
X_START, X_MID, X_FINE, X_GHOST, X_BRICK, X_ROWS = 0, 24, 88, 152, 160, 168


def iota(shape, dim):
    return lax.broadcasted_iota(jnp.int32, shape, dim)


def onehot(mask):
    return jnp.where(mask, 1.0, 0.0).astype(F32)


def dot(a, b):
    return jnp.dot(a, b, precision=HI, preferred_element_type=F32)


def turn(v, shift):
    shift = shift % LANES
    return v if shift == 0 else pltpu.roll(v, shift, v.ndim - 1)


def y_sum(tiles):
    n = len(tiles)
    sub = iota((8, LANES), 0)
    first = jnp.where(sub == 0, 0.0, pltpu.roll(tiles[n - 1], 1, 0))
    last = jnp.where(sub == 7, 0.0, pltpu.roll(tiles[0], 7, 0))
    up = [first] + tiles[:-1]
    down = tiles[1:] + [last]
    return [a + b for a, b in zip(up, down)]


def along_y(tiles, z_sums):
    four = [4.0 * v for v in tiles]
    a = [v + z for v, z in zip(four, z_sums)]
    b = [v + y for v, y in zip(four, y_sum(tiles))]
    c = [4.0 * v + y for v, y in zip(a, y_sum(a))]
    return [x + y for x, y in zip(a, b)], c


def relax(v, rhs, inverse, weight, d, e, c):
    return v + inverse * ((rhs - (c + d)) - weight * e)


def along_x(before, here, after):
    return 4.0 * here + (before + after)


def pack_z(
    src_hbm, occ_hbm, cls_hbm, tab_hbm, par_hbm, co_hbm, za, zb, co_out, pown, fine,
    src, occ, cls, tab, par, co, zl, zr, sems,
):
    copies = [
        pltpu.make_async_copy(a, b, sems.at[i])
        for i, (a, b) in enumerate(
            ((occ_hbm, occ), (cls_hbm, cls), (tab_hbm, tab), (par_hbm, par), (co_hbm, co), (src_hbm, src))
        )
    ]
    for copy in copies:
        copy.start()
    slab = lax.axis_index("slab")
    first = (slab - 1) * COARSE
    for copy in copies[:-1]:
        copy.wait()
    for t in range(4):
        part = co[0, :, LANES * t : LANES * (t + 1)]
        zl[Z_COARSE + 4 * t : Z_COARSE + 4 * t + 4, :] = part
        co_out[4 * t : 4 * t + 4, :] = part
    zr[Z_COARSE : Z_COARSE + 16, :] = zl[Z_COARSE : Z_COARSE + 16, :]
    zl[Z_POS : Z_POS + 8, :] = jnp.full((8, LANES), par[0, 0, 0] - first, jnp.int32).astype(F32)
    zr[Z_POS : Z_POS + 8, :] = jnp.full((8, LANES), par[0, 0, 7] - first, jnp.int32).astype(F32)
    pown[...] = jnp.zeros((64, LANES), F32)
    for bx in range(4):
        occupied = occ[bx].astype(F32)
        labels = cls[bx]
        weight = jnp.zeros((4, 16), F32)
        for c in range(16):
            weight = weight + jnp.where(labels == c, tab[c], 0.0)
        screen = screen_strength * weight
        inverse = occupied / (stiff_diagonal + screen * mass_diagonal)
        for parity in range(2):
            pown[pl.ds(8 * bx + parity, 4, 2), 0:16] = inverse
            pown[pl.ds(32 + 8 * bx + parity, 4, 2), 0:16] = screen
    lane = iota((8, LANES), 1)
    packed = jnp.zeros((8, LANES), F32)
    for q in range(8):
        packed = jnp.where(lane // 16 == q, turn(pown[8 * q : 8 * q + 8, :], 16 * q), packed)
    zl[Z_BRICK : Z_BRICK + 8, :] = packed
    zr[Z_BRICK : Z_BRICK + 8, :] = packed
    copies[-1].wait()
    slot = lane // 8
    for g in range(2):
        for t in range(4):
            left = jnp.zeros((8, LANES), F32)
            right = jnp.zeros((8, LANES), F32)
            for i in range(16):
                v = 6.0 * src[16 * g + i, pl.ds(t, 8, 4), :]
                fine[16 * g + i, 8 * t : 8 * t + 8, :] = v
                left = jnp.where(slot == i, turn(v, 8 * i), left)
                right = jnp.where(slot == i, turn(v, 8 * i + 8), right)
            row = Z_SRC + 32 * g + 8 * t
            zl[row : row + 8, :] = left
            zr[row : row + 8, :] = right
    even = slab % 2 == 0
    za[...] = jnp.where(even, zr[...], zl[...])
    zb[...] = jnp.where(even, zl[...], zr[...])


def extend_z(
    fine, par, co, pown, ha, hb, fc, fd, xa, xb, start, mid, ghost, bricks, cand, pairs, hl, hr, xl, xr
):
    slab = lax.axis_index("slab")
    first = (slab - 2) * COARSE
    even = slab % 2 == 0
    hl[...] = jnp.where(even, hb[...], ha[...])
    hr[...] = jnp.where(even, ha[...], hb[...])

    @pl.when(slab == 0)
    def _():
        hl[Z_BRICK : Z_BRICK + 8, :] = jnp.zeros((8, LANES), F32)

    @pl.when(slab == lax.axis_size("slab") - 1)
    def _():
        hr[Z_BRICK : Z_BRICK + 8, :] = jnp.zeros((8, LANES), F32)

    near = slab % 4 < 2
    cand[20:24, :] = jnp.zeros((4, 512), F32)
    cand[8:12, :] = co[0]
    for t in range(4):
        c, d = fc[4 * t : 4 * t + 4, :], fd[4 * t : 4 * t + 4, :]
        cand[0:4, LANES * t : LANES * (t + 1)] = jnp.where(near, d, c)
        cand[16:20, LANES * t : LANES * (t + 1)] = jnp.where(near, c, d)
        cand[4:8, LANES * t : LANES * (t + 1)] = hl[Z_COARSE + 4 * t : Z_COARSE + 4 * t + 4, :]
        cand[12:16, LANES * t : LANES * (t + 1)] = hr[Z_COARSE + 4 * t : Z_COARSE + 4 * t + 4, :]
    sub, lane = iota((8, LANES), 0), iota((8, LANES), 1)
    chosen = jnp.full((8, LANES), -1, jnp.int32)
    for k in range(4):
        chosen = jnp.where(sub == k + 1, par[0, 0, 2 * k] - first, chosen)
    chosen = chosen.astype(F32)
    chosen = jnp.where(sub == 0, hl[Z_POS : Z_POS + 8, :], chosen)
    chosen = jnp.where(sub == 5, hr[Z_POS : Z_POS + 8, :] + 2.0 * COARSE, chosen)
    pick = onehot(chosen == lane.astype(F32))
    six = dot(pick[:, 0:24], cand[...])
    row2, lane2 = iota((16, LANES), 0), iota((16, LANES), 1)
    spread = onehot(lane2 // 8 == row2)
    c, z = iota((LANES, LANES), 0), iota((LANES, LANES), 1)
    place = onehot(c % 8 == z % 16 // 2)
    zone = lane2 // 16
    rows = jnp.concatenate(
        [
            jnp.broadcast_to(six[k : k + 1, LANES * t : LANES * (t + 1)], (16, LANES)) * spread
            for t in range(4)
            for k in range(6)
        ],
        axis=0,
    )
    placed = dot(rows, place)
    for t in range(4):
        total = jnp.zeros((16, LANES), F32)
        for k in range(6):
            at = 16 * (6 * t + k)
            total = jnp.where(zone == (7 if k == 0 else k - 1), placed[at : at + 16], total)
        start[16 * t : 16 * (t + 1), :] = total
    for q in range(8):
        low = turn(hl[Z_BRICK : Z_BRICK + 8, :], 112 - 16 * q)
        high = turn(hr[Z_BRICK : Z_BRICK + 8, :], 16 - 16 * q)
        own = pown[8 * q : 8 * q + 8, :]
        bricks[8 * q : 8 * q + 8, :] = jnp.where(lane >= 126, low, jnp.where(lane // 2 == 8, high, own))
    for g in range(2):
        for t in range(4):
            row = Z_SRC + 32 * g + 8 * t
            low, high = turn(hl[row : row + 8, :], -4), turn(hr[row : row + 8, :], 4)
            ghost[32 * g + 8 * t : 32 * g + 8 * t + 8, :] = jnp.where(lane % 8 < 4, low, high)
    z2, l2 = iota((2 * LANES, LANES), 0), iota((2 * LANES, LANES), 1)
    join = (z2 < 128) & (z2 // 2 == l2)
    join = join | ((z2 >= 128) & (z2 < 136) & (l2 == 64 + (z2 - 128) // 2))
    join = join | ((z2 >= 248) & (l2 == z2 // 2))
    join = onehot(join)
    for g in range(2):
        for u in range(2):
            row = Z_SRC + 32 * g + 16 * u
            low = hl[row : row + 8, :] + hl[row + 8 : row + 16, :]
            high = hr[row : row + 8, :] + hr[row + 8 : row + 16, :]
            low, high = low + turn(low, -8), high + turn(high, -8)
            for i in range(8):
                x, at = 2 * (8 * g + i), 16 * (8 * g + i) + 8 * u
                pairs[at : at + 8, 0:LANES] = (
                    fine[x, 16 * u : 16 * u + 8, :]
                    + fine[x, 16 * u + 8 : 16 * u + 16, :]
                    + fine[x + 1, 16 * u : 16 * u + 8, :]
                    + fine[x + 1, 16 * u + 8 : 16 * u + 16, :]
                )
                pairs[at : at + 8, LANES:] = jnp.where(
                    lane < 8, turn(high, -16 * i), jnp.where(lane >= 120, turn(low, 120 - 16 * i), 0.0)
                )
    summed = 0.25 * dot(pairs[...], join)
    for i in range(16):
        mid[i] = summed[16 * i : 16 * (i + 1)]
    for out, rows, m0, f0, g0, b0, edge in ((xl, 0, 0, 0, 0, 0, 0), (xr, 40, 12, 30, 1, 2, 16)):
        out[X_START : X_START + 24, :] = start[rows : rows + 24, :]
        for i in range(4):
            out[X_MID + 16 * i : X_MID + 16 * (i + 1), :] = mid[m0 + i]
        for i in range(2):
            out[X_FINE + NY * i : X_FINE + NY * (i + 1), :] = fine[f0 + i]
        packed = jnp.zeros((8, LANES), F32)
        boxes = jnp.zeros((8, LANES), F32)
        for t in range(4):
            v = ghost[32 * g0 + 8 * t : 32 * g0 + 8 * t + 8, :]
            packed = jnp.where(lane // 16 == t, turn(v, 16 * t + edge), packed)
            at = 32 * (t // 2) + 8 * (b0 + t % 2)
            boxes = jnp.where(lane // 32 == t, turn(bricks[at : at + 8, :], 32 * t + 2), boxes)
        out[X_GHOST : X_GHOST + 8, :] = packed
        out[X_BRICK : X_BRICK + 8, :] = boxes
    grp_even = lax.axis_index("grp") % 2 == 0
    xa[...] = jnp.where(grp_even, xr[...], xl[...])
    xb[...] = jnp.where(grp_even, xl[...], xr[...])


def sweep_all(
    fine, xa, xb, start, smid, sghost, bricks, mid_hbm, fin_hbm,
    v13, pext, coef, rep, m1, m2, xl, xr, mid_out, fin_out, sems,
):
    grp = lax.axis_index("grp")
    even = grp % 2 == 0
    xl[...] = jnp.where(even, xb[...], xa[...])
    xr[...] = jnp.where(even, xa[...], xb[...])

    @pl.when(grp == 0)
    def _():
        xl[X_BRICK : X_BRICK + 8, :] = jnp.zeros((8, LANES), F32)

    @pl.when(grp == lax.axis_size("grp") - 1)
    def _():
        xr[X_BRICK : X_BRICK + 8, :] = jnp.zeros((8, LANES), F32)

    lane = iota((8, LANES), 1)
    ring = (lane < 18) | (lane >= 126)
    for field in range(2):
        pext[64 * field + 16 : 64 * field + 48, :] = bricks[32 * field : 32 * field + 32, :]
        for b in range(2):
            shift = -(32 * (2 * field + b) + 2)
            at = 64 * field + 8 * b
            pext[at : at + 8, :] = jnp.where(ring, turn(xl[X_BRICK : X_BRICK + 8, :], shift), 0.0)
            pext[at + 48 : at + 56, :] = jnp.where(ring, turn(xr[X_BRICK : X_BRICK + 8, :], shift), 0.0)
    b, l = iota((LANES, 3 * LANES), 0), iota((LANES, 3 * LANES), 1)
    z = l % LANES
    hit = (l < 128) & (b == jnp.where(z >= 96, z // 4 + 96, z // 4))
    hit = hit | ((l >= 128) & (l < 256) & (b == z // 8))
    hit = hit | ((l >= 256) & (b == jnp.where(z % 8 < 4, 127, 16)))
    spread = dot(pext[...], onehot(hit))
    coef[0:64, :] = spread[0:64] * (relaxation / 6.0)
    coef[64:128, :] = spread[64:128] * (1.0 / 36.0) - 0.5

    def inverse13(bx):
        return coef[8 * (bx + 2) : 8 * (bx + 3), 0:LANES]

    def weight13(bx):
        return coef[64 + 8 * (bx + 2) : 72 + 8 * (bx + 2), 0:LANES]

    def inverse14(bx):
        return coef[8 * (bx + 2) : 8 * (bx + 3), LANES : 2 * LANES]

    def weight14(bx):
        return coef[64 + 8 * (bx + 2) : 72 + 8 * (bx + 2), LANES : 2 * LANES]

    for x in range(-5, 21):
        q = x // 2
        if q < 0:
            v = xl[X_START + 8 * (q + 3) : X_START + 8 * (q + 4), :]
        elif q > 7:
            v = xr[X_START + 8 * (q - 8) : X_START + 8 * (q - 7), :]
        else:
            v = start[8 * q : 8 * q + 8, :]
        v = jnp.where(inverse13(x // 4) != 0.0, v, 0.0)
        v13[x + 5, 0:8, :] = v
        v13[x + 5, 8:16, :] = v

    def rhs13(x, u):
        if x < 0:
            return xl[X_MID + 16 * (x + 4) + 8 * u : X_MID + 16 * (x + 4) + 8 * u + 8, :]
        if x > 15:
            return xr[X_MID + 16 * (x - 16) + 8 * u : X_MID + 16 * (x - 16) + 8 * u + 8, :]
        return smid[x, 8 * u : 8 * u + 8, :]

    for n in range(SWEEPS):
        low, high = -4 + n, 19 - n
        planes = {}
        for x in range(low - 1, high + 2):
            tiles = [v13[x + 5, 8 * u : 8 * u + 8, :] for u in range(2)]
            planes[x] = along_y(tiles, [turn(v, 1) + turn(v, -1) for v in tiles])
            if x > low:
                o = x - 1
                for u in range(2):
                    d = along_x(planes[o - 1][0][u], planes[o][0][u], planes[x][0][u])
                    e = along_x(planes[o - 1][1][u], planes[o][1][u], planes[x][1][u])
                    v13[o + 5, 8 * u : 8 * u + 8, :] = relax(
                        v13[o + 5, 8 * u : 8 * u + 8, :],
                        rhs13(o, u), inverse13(o // 4), weight13(o // 4), d, e, planes[o][1][u],
                    )
    for x in range(16):
        for u in range(2):
            mid_out[x, pl.ds(u, 8, 2), :] = v13[x + 5, 8 * u : 8 * u + 8, 0:64]
    mid_copy = pltpu.make_async_copy(mid_out, mid_hbm, sems.at[0])
    mid_copy.start()

    b, l = iota((LANES, 3 * LANES), 0), iota((LANES, 3 * LANES), 1)
    j = l % 8
    hit = (l < 128) & (b == l // 2)
    hit = hit | ((l >= 128) & (l < 256) & (b == jnp.where(j < 4, 126 + j // 2, 62 + j // 2)))
    hit = hit | ((l >= 256) & (b == jnp.where(j < 4, 63, 0)))
    parents = jnp.concatenate(
        [
            jnp.where(inverse13(x // 4) != 0.0, v13[x + 5, 8 * u : 8 * u + 8, :], 0.0)
            for x in range(-2, 18)
            for u in range(2)
        ],
        axis=0,
    )
    rep[...] = dot(parents, onehot(hit))

    def parent(q, u):
        return rep[16 * (q + 2) + 8 * u : 16 * (q + 2) + 8 * u + 8, 0:LANES]

    zero = jnp.zeros((8, LANES), F32)
    halo = [[zero, zero] for _ in range(4)]
    for q in range(-2, 18):
        g, i = q // 8 + 1, q % 8
        for u in range(2):
            v = rep[16 * (q + 2) + 8 * u : 16 * (q + 2) + 8 * u + 8, LANES : 2 * LANES]
            halo[g][u] = jnp.where(lane // 16 == i, v, halo[g][u])
    halo = [[tiles[t // 2] for t in range(4)] for tiles in halo]
    halo_rhs, halo_inverse, halo_weight = [], [], []
    for g in range(4):
        if g == 0:
            packed = xl[X_GHOST : X_GHOST + 8, :]
            halo_rhs.append([turn(packed, 112 - 16 * t) for t in range(4)])
        elif g == 3:
            packed = xr[X_GHOST : X_GHOST + 8, :]
            halo_rhs.append([turn(packed, -16 * t) for t in range(4)])
        else:
            halo_rhs.append([sghost[32 * (g - 1) + 8 * t : 32 * (g - 1) + 8 * t + 8, :] for t in range(4)])
        for field, out in ((0, halo_inverse), (64, halo_weight)):
            one, two = (coef[field + 8 * (2 * g + k) : field + 8 * (2 * g + k) + 8, 2 * LANES :] for k in range(2))
            out.append(jnp.where(lane < 64, one, two))

    def z_main(v, halo_tile, i):
        edge = turn(halo_tile, -(8 * i + 4))
        return turn(jnp.where(lane == 127, edge, v), 1) + turn(jnp.where(lane == 0, edge, v), -1)

    def sweep_halo(halo, edges):
        planes = []
        for g in range(4):
            right = [jnp.where(lane % 8 == 3, e, v) for e, v in zip(edges[g], halo[g])]
            left = [jnp.where(lane % 8 == 4, e, v) for e, v in zip(edges[g], halo[g])]
            planes.append(along_y(halo[g], [turn(r, 1) + turn(v, -1) for r, v in zip(right, left)]))
        moved = [[[(turn(v, 8), turn(v, -8)) for v in part] for part in plane] for plane in planes]
        out = []
        for g in range(4):
            tiles = []
            for t in range(4):
                de = []
                for part in range(2):
                    before, after = moved[g][part][t]
                    if g > 0:
                        before = jnp.where(lane < 8, moved[g - 1][part][t][0], before)
                    if g < 3:
                        after = jnp.where(lane >= 120, moved[g + 1][part][t][1], after)
                    de.append(along_x(before, planes[g][part][t], after))
                tiles.append(
                    relax(
                        halo[g][t], halo_rhs[g][t], halo_inverse[g], halo_weight[g],
                        de[0], de[1], planes[g][1][t],
                    )
                )
            out.append(tiles)
        return out

    def rhs14(x, t):
        if x < 0:
            return xl[X_FINE + NY * (x + 2) + 8 * t : X_FINE + NY * (x + 2) + 8 * t + 8, :]
        if x > 31:
            return xr[X_FINE + NY * (x - 32) + 8 * t : X_FINE + NY * (x - 32) + 8 * t + 8, :]
        return fine[x, 8 * t : 8 * t + 8, :]

    edges = [[zero, zero] for _ in range(4)]
    for q in range(-2, 18):
        g, i = q // 8 + 1, q % 8
        for u in range(2):
            v = rep[16 * (q + 2) + 8 * u : 16 * (q + 2) + 8 * u + 8, 2 * LANES :]
            edges[g][u] = jnp.where(lane // 16 == i, v, edges[g][u])
    edges = [[tiles[t // 2] for t in range(4)] for tiles in edges]
    planes = {}
    for q in range(-2, 18):
        g, i = (2 * q) // 16 + 1, (2 * q) % 16
        tiles = [parent(q, u) for u in range(2)]
        sums = [z_main(tiles[u], halo[g][2 * u], i) for u in range(2)]
        planes[q] = along_y([tiles[t // 2] for t in range(4)], [sums[t // 2] for t in range(4)])
        o = q - 1
        if o >= -1:
            for t in range(4):
                f5, c5 = 5.0 * planes[o][0][t], 5.0 * planes[o][1][t]
                for child in range(2):
                    x, near = 2 * o + child, o - 1 + 2 * child
                    d, e = f5 + planes[near][0][t], c5 + planes[near][1][t]
                    m1[x + 3, 8 * t : 8 * t + 8, :] = relax(
                        parent(o, t // 2), rhs14(x, t), inverse14(x // 8), weight14(x // 8),
                        d, e, planes[o][1][t],
                    )
    halo = sweep_halo(halo, edges)

    pieces = []
    for n, source, target in ((1, m1, m2), (2, m2, None)):
        low, high = -2 + n, 33 - n
        if n == 1:
            edges = [[zero] * 4 for _ in range(4)]
            b, l = iota((LANES, LANES), 0), iota((LANES, LANES), 1)
            hit = ((b == 127) & (l % 8 == 3)) | ((b == 0) & (l % 8 == 4))
            wide = [source[x + 3] for x in range(low - 1, high + 2)]
            wide = dot(jnp.concatenate(wide, axis=0), onehot(hit))
            for x in range(low - 1, high + 2):
                g, i = x // 16 + 1, x % 16
                for t in range(4):
                    at = 32 * (x - low + 1) + 8 * t
                    edges[g][t] = jnp.where(lane // 8 == i, wide[at : at + 8], edges[g][t])
        planes = {}
        for x in range(low - 1, high + 2):
            g, i = x // 16 + 1, x % 16
            tiles = [source[x + 3, 8 * t : 8 * t + 8, :] for t in range(4)]
            planes[x] = along_y(tiles, [z_main(tiles[t], halo[g][t], i) for t in range(4)])
            if x > low:
                o = x - 1
                for t in range(4):
                    d = along_x(planes[o - 1][0][t], planes[o][0][t], planes[x][0][t])
                    e = along_x(planes[o - 1][1][t], planes[o][1][t], planes[x][1][t])
                    value = relax(
                        source[o + 3, 8 * t : 8 * t + 8, :],
                        rhs14(o, t), inverse14(o // 8), weight14(o // 8), d, e, planes[o][1][t],
                    )
                    if target is None:
                        fin_out[o, pl.ds(t, 8, 4), :] = value
                    else:
                        target[o + 3, 8 * t : 8 * t + 8, :] = value
                if target is None and o % 8 == 7:
                    part = pl.ds(o - 7, 8)
                    pieces.append(pltpu.make_async_copy(fin_out.at[part], fin_hbm.at[part], sems.at[1 + o // 8]))
                    pieces[-1].start()
        if n == 1:
            halo = sweep_halo(halo, edges)
    mid_copy.wait()
    for piece in pieces:
        piece.wait()


def pairing(couples):
    partner = {}
    for a, b in couples:
        partner[a], partner[b] = b, a
    return sorted(partner.items())


def pairings(groups, slabs):
    def at(g, s):
        return g * slabs + s

    every = range(groups)
    one = [(at(g, s), at(g, s + 1)) for g in every for s in range(0, slabs, 2)]
    two = [(at(g, s), at(g, s + 1)) for g in every for s in range(1, slabs - 1, 2)]
    two += [(at(g, s), at(g + 1, s)) for g in range(0, groups, 2) for s in (0, slabs - 1)]
    three = [(at(g, s), at(g, s + 2)) for g in every for s in range(slabs) if s % 4 < 2]
    four = [(at(g, s), at(g, s + 2)) for g in every for s in range(slabs - 2) if s % 4 >= 2]
    four += [(at(g, s), at(g, s + 1)) for g in every for s in (0, slabs - 2)]
    five = [(at(g, s), at(g + 1, s)) for g in range(0, groups, 2) for s in range(slabs)]
    six = [(at(g, s), at(g + 1, s)) for g in range(1, groups - 1, 2) for s in range(slabs)]
    six += [(at(g, s), at(g, s + 1)) for g in (0, groups - 1) for s in range(0, slabs, 2)]
    return [pairing(couples) for couples in (one, two, three, four, five, six)]


def build(mesh, interpret=False):
    one, two, three, four, five, six = pairings(mesh.shape["grp"], mesh.shape["slab"])

    def local(source, occupancy, classes, screen_table, parents, coarse):
        def sds(*shape):
            return jax.ShapeDtypeStruct(shape, F32)

        vm = pl.BlockSpec(memory_space=VMEM)
        sm = pl.BlockSpec(memory_space=SMEM)
        hbm = pl.BlockSpec(memory_space=pltpu.HBM)

        def swap(block, pairs):
            return lax.ppermute(block, ("grp", "slab"), pairs)

        za, zb, rows, pown, fine = pl.pallas_call(
            pack_z,
            out_shape=(
                sds(Z_ROWS, LANES), sds(Z_ROWS, LANES), sds(16, LANES), sds(64, LANES), sds(CX, NY, LANES),
            ),
            in_specs=[hbm] * 6,
            out_specs=(vm,) * 5,
            scratch_shapes=[
                VMEM((CX, NY, LANES), F32),
                VMEM((4, 4, 16), jnp.int32),
                VMEM((4, 4, 16), jnp.int32),
                SMEM((16,), F32),
                SMEM((2, 2, 8), jnp.int32),
                VMEM((1, 4, 512), F32),
                VMEM((Z_ROWS, LANES), F32),
                VMEM((Z_ROWS, LANES), F32),
                pltpu.SemaphoreType.DMA((6,)),
            ],
            interpret=interpret,
            compiler_params=pltpu.CompilerParams(vmem_limit_bytes=4 << 20),
            name="pack_z",
        )(*(pltpu.with_memory_space_constraint(x, pltpu.HBM) for x in (source, occupancy, classes, screen_table, parents, coarse)))
        ha = swap(za, one)
        hb = swap(zb, two)
        fc = swap(rows, three)
        fd = swap(rows, four)
        xa, xb, start, mid, ghost, bricks = pl.pallas_call(
            extend_z,
            out_shape=(
                sds(X_ROWS, LANES), sds(X_ROWS, LANES), sds(64, LANES), sds(16, 16, LANES),
                sds(64, LANES), sds(64, LANES),
            ),
            in_specs=[vm, sm] + [vm] * 6,
            out_specs=(vm,) * 6,
            scratch_shapes=[
                VMEM((24, 512), F32),
                VMEM((256, 2 * LANES), F32),
                VMEM((Z_ROWS, LANES), F32),
                VMEM((Z_ROWS, LANES), F32),
                VMEM((X_ROWS, LANES), F32),
                VMEM((X_ROWS, LANES), F32),
            ],
            interpret=interpret,
            compiler_params=pltpu.CompilerParams(vmem_limit_bytes=8 << 20),
            name="extend_z",
        )(fine, parents, coarse, pown, ha, hb, fc, fd)
        ga = swap(xa, five)
        gb = swap(xb, six)
        return pl.pallas_call(
            sweep_all,
            out_shape=(sds(16, 16, 64), sds(CX, NY, CZ)),
            in_specs=[vm] * 7,
            out_specs=(hbm, hbm),
            scratch_shapes=[
                VMEM((26, 16, LANES), F32),
                VMEM((LANES, LANES), F32),
                VMEM((LANES, 3 * LANES), F32),
                VMEM((320, 3 * LANES), F32),
                VMEM((38, NY, LANES), F32),
                VMEM((38, NY, LANES), F32),
                VMEM((X_ROWS, LANES), F32),
                VMEM((X_ROWS, LANES), F32),
                VMEM((16, 16, 64), F32),
                VMEM((CX, NY, LANES), F32),
                pltpu.SemaphoreType.DMA((5,)),
            ],
            interpret=interpret,
            compiler_params=pltpu.CompilerParams(vmem_limit_bytes=16 << 20),
            name="sweep_all",
        )(fine, ga, gb, start, mid, ghost, bricks)

    return local


def solution(mesh, interpret=False):
    placed = (
        P("grp", None, "slab"),
        P("grp", None, "slab"),
        P("grp", None, "slab"),
        P(),
        P("grp", None, "slab"),
        P("grp", "slab", None),
    )
    return jax.shard_map(
        build(mesh, interpret),
        mesh=mesh,
        in_specs=placed,
        out_specs=(P("grp", None, "slab"), P("grp", None, "slab")),
        check_vma=False,
    )
```

```python
import jax
import jax.numpy as jnp
from jax import lax
from jax.experimental import pallas as pl
from jax.experimental.pallas import tpu as pltpu
from jax.sharding import PartitionSpec as P

SWEEPS = 3

screen_strength = 4.0
relaxation = 2.0 / 3.0
stiff_diagonal = 8.0 / 3.0
mass_diagonal = 8.0 / 27.0

F32 = jnp.float32
HI = lax.Precision.HIGHEST
VMEM = pltpu.VMEM
SMEM = pltpu.SMEM

CX, NY, CZ = 32, 32, 128
LANES = 128
COARSE = 4

Z_COARSE, Z_POS, Z_BRICK, Z_SRC, Z_ROWS = 0, 16, 24, 32, 96
X_START, X_MID, X_FINE, X_GHOST, X_BRICK, X_ROWS = 0, 24, 64, 128, 136, 144


def iota(shape, dim):
    return lax.broadcasted_iota(jnp.int32, shape, dim)


def onehot(mask):
    return jnp.where(mask, 1.0, 0.0).astype(F32)


def dot(a, b):
    return jnp.dot(a, b, precision=HI, preferred_element_type=F32)


def turn(v, shift):
    shift = shift % LANES
    return v if shift == 0 else pltpu.roll(v, shift, v.ndim - 1)


def y_sum(tiles):
    n = len(tiles)
    sub = iota((8, LANES), 0)
    first = jnp.where(sub == 0, 0.0, pltpu.roll(tiles[n - 1], 1, 0))
    last = jnp.where(sub == 7, 0.0, pltpu.roll(tiles[0], 7, 0))
    up = [first] + tiles[:-1]
    down = tiles[1:] + [last]
    return [a + b for a, b in zip(up, down)]


def along_y(tiles, z_sums):
    four = [4.0 * v for v in tiles]
    a = [v + z for v, z in zip(four, z_sums)]
    b = [v + y for v, y in zip(four, y_sum(tiles))]
    c = [4.0 * v + y for v, y in zip(a, y_sum(a))]
    return [x + y for x, y in zip(a, b)], c


def relax(v, rhs, inverse, weight, d, e, c):
    return v + inverse * ((rhs - (c + d)) - weight * e)


def along_x(before, here, after):
    return 4.0 * here + (before + after)


def pack_z(
    src_hbm, occ_hbm, cls_hbm, tab_hbm, par_hbm, co_hbm, za, zb, co_out, pown, fine,
    src, occ, cls, tab, par, co, zl, zr, sems,
):
    copies = [
        pltpu.make_async_copy(a, b, sems.at[i])
        for i, (a, b) in enumerate(
            ((occ_hbm, occ), (cls_hbm, cls), (tab_hbm, tab), (par_hbm, par), (co_hbm, co), (src_hbm, src))
        )
    ]
    for copy in copies:
        copy.start()
    slab = lax.axis_index("slab")
    first = (slab - 1) * COARSE
    for copy in copies[:-1]:
        copy.wait()
    for t in range(4):
        part = co[0, :, LANES * t : LANES * (t + 1)]
        zl[Z_COARSE + 4 * t : Z_COARSE + 4 * t + 4, :] = part
        co_out[4 * t : 4 * t + 4, :] = part
    zr[Z_COARSE : Z_COARSE + 16, :] = zl[Z_COARSE : Z_COARSE + 16, :]
    zl[Z_POS : Z_POS + 8, :] = jnp.full((8, LANES), par[0, 0, 0] - first, jnp.int32).astype(F32)
    zr[Z_POS : Z_POS + 8, :] = jnp.full((8, LANES), par[0, 0, 7] - first, jnp.int32).astype(F32)
    pown[...] = jnp.zeros((64, LANES), F32)
    for bx in range(4):
        occupied = occ[bx].astype(F32)
        labels = cls[bx]
        weight = jnp.zeros((4, 16), F32)
        for c in range(16):
            weight = weight + jnp.where(labels == c, tab[c], 0.0)
        screen = screen_strength * weight
        inverse = occupied / (stiff_diagonal + screen * mass_diagonal)
        for parity in range(2):
            pown[pl.ds(8 * bx + parity, 4, 2), 0:16] = inverse
            pown[pl.ds(32 + 8 * bx + parity, 4, 2), 0:16] = screen
    lane = iota((8, LANES), 1)
    packed = jnp.zeros((8, LANES), F32)
    for q in range(8):
        packed = jnp.where(lane // 16 == q, turn(pown[8 * q : 8 * q + 8, :], 16 * q), packed)
    zl[Z_BRICK : Z_BRICK + 8, :] = packed
    zr[Z_BRICK : Z_BRICK + 8, :] = packed
    copies[-1].wait()
    slot = lane // 8
    for g in range(2):
        for t in range(4):
            left = jnp.zeros((8, LANES), F32)
            right = jnp.zeros((8, LANES), F32)
            for i in range(16):
                v = 6.0 * src[16 * g + i, pl.ds(t, 8, 4), :]
                fine[16 * g + i, 8 * t : 8 * t + 8, :] = v
                left = jnp.where(slot == i, turn(v, 8 * i), left)
                right = jnp.where(slot == i, turn(v, 8 * i + 8), right)
            row = Z_SRC + 32 * g + 8 * t
            zl[row : row + 8, :] = left
            zr[row : row + 8, :] = right
    even = slab % 2 == 0
    za[...] = jnp.where(even, zr[...], zl[...])
    zb[...] = jnp.where(even, zl[...], zr[...])


def extend_z(
    fine, par, co, pown, ha, hb, fc, fd, xa, xb, start, mid, ghost, bricks, cand, pairs, hl, hr, xl, xr
):
    slab = lax.axis_index("slab")
    first = (slab - 2) * COARSE
    even = slab % 2 == 0
    hl[...] = jnp.where(even, hb[...], ha[...])
    hr[...] = jnp.where(even, ha[...], hb[...])

    @pl.when(slab == 0)
    def _():
        hl[Z_BRICK : Z_BRICK + 8, :] = jnp.zeros((8, LANES), F32)

    @pl.when(slab == lax.axis_size("slab") - 1)
    def _():
        hr[Z_BRICK : Z_BRICK + 8, :] = jnp.zeros((8, LANES), F32)

    near = slab % 4 < 2
    cand[20:24, :] = jnp.zeros((4, 512), F32)
    cand[8:12, :] = co[0]
    for t in range(4):
        c, d = fc[4 * t : 4 * t + 4, :], fd[4 * t : 4 * t + 4, :]
        cand[0:4, LANES * t : LANES * (t + 1)] = jnp.where(near, d, c)
        cand[16:20, LANES * t : LANES * (t + 1)] = jnp.where(near, c, d)
        cand[4:8, LANES * t : LANES * (t + 1)] = hl[Z_COARSE + 4 * t : Z_COARSE + 4 * t + 4, :]
        cand[12:16, LANES * t : LANES * (t + 1)] = hr[Z_COARSE + 4 * t : Z_COARSE + 4 * t + 4, :]
    sub, lane = iota((8, LANES), 0), iota((8, LANES), 1)
    chosen = jnp.full((8, LANES), -1, jnp.int32)
    for k in range(4):
        chosen = jnp.where(sub == k + 1, par[0, 0, 2 * k] - first, chosen)
    chosen = chosen.astype(F32)
    chosen = jnp.where(sub == 0, hl[Z_POS : Z_POS + 8, :], chosen)
    chosen = jnp.where(sub == 5, hr[Z_POS : Z_POS + 8, :] + 2.0 * COARSE, chosen)
    pick = onehot(chosen == lane.astype(F32))
    six = dot(pick[:, 0:24], cand[...])
    row2, lane2 = iota((16, LANES), 0), iota((16, LANES), 1)
    spread = onehot(lane2 // 8 == row2)
    c, z = iota((LANES, LANES), 0), iota((LANES, LANES), 1)
    place = onehot(c % 8 == z % 16 // 2)
    zone = lane2 // 16
    rows = jnp.concatenate(
        [
            jnp.broadcast_to(six[k : k + 1, LANES * t : LANES * (t + 1)], (16, LANES)) * spread
            for t in range(4)
            for k in range(6)
        ],
        axis=0,
    )
    placed = dot(rows, place)
    for t in range(4):
        total = jnp.zeros((16, LANES), F32)
        for k in range(6):
            at = 16 * (6 * t + k)
            total = jnp.where(zone == (7 if k == 0 else k - 1), placed[at : at + 16], total)
        start[16 * t : 16 * (t + 1), :] = total
    for q in range(8):
        low = turn(hl[Z_BRICK : Z_BRICK + 8, :], 112 - 16 * q)
        high = turn(hr[Z_BRICK : Z_BRICK + 8, :], 16 - 16 * q)
        own = pown[8 * q : 8 * q + 8, :]
        bricks[8 * q : 8 * q + 8, :] = jnp.where(lane >= 126, low, jnp.where(lane // 2 == 8, high, own))
    for g in range(2):
        for t in range(4):
            row = Z_SRC + 32 * g + 8 * t
            low, high = turn(hl[row : row + 8, :], -4), turn(hr[row : row + 8, :], 4)
            ghost[32 * g + 8 * t : 32 * g + 8 * t + 8, :] = jnp.where(lane % 8 < 4, low, high)
    z2, l2 = iota((2 * LANES, LANES), 0), iota((2 * LANES, LANES), 1)
    join = (z2 < 128) & (z2 // 2 == l2)
    join = join | ((z2 >= 128) & (z2 < 136) & (l2 == 64 + (z2 - 128) // 2))
    join = join | ((z2 >= 248) & (l2 == z2 // 2))
    join = onehot(join)
    for g in range(2):
        for u in range(2):
            row = Z_SRC + 32 * g + 16 * u
            low = hl[row : row + 8, :] + hl[row + 8 : row + 16, :]
            high = hr[row : row + 8, :] + hr[row + 8 : row + 16, :]
            low, high = low + turn(low, -8), high + turn(high, -8)
            for i in range(8):
                x, at = 2 * (8 * g + i), 16 * (8 * g + i) + 8 * u
                pairs[at : at + 8, 0:LANES] = (
                    fine[x, 16 * u : 16 * u + 8, :]
                    + fine[x, 16 * u + 8 : 16 * u + 16, :]
                    + fine[x + 1, 16 * u : 16 * u + 8, :]
                    + fine[x + 1, 16 * u + 8 : 16 * u + 16, :]
                )
                pairs[at : at + 8, LANES:] = jnp.where(
                    lane < 8, turn(high, -16 * i), jnp.where(lane >= 120, turn(low, 120 - 16 * i), 0.0)
                )
    summed = 0.25 * dot(pairs[...], join)
    for i in range(16):
        mid[i] = summed[16 * i : 16 * (i + 1)]
    for out, rows, m0, f0, g0, b0, edge in ((xl, 0, 0, 0, 0, 0, 0), (xr, 40, 12, 30, 1, 2, 16)):
        out[X_START : X_START + 24, :] = start[rows : rows + 24, :]
        sides = jnp.zeros((8, LANES), F32)
        for i in range(4):
            for u in range(2):
                v = mid[m0 + i, 8 * u : 8 * u + 8, :]
                sides = jnp.where(lane % 64 // 8 == 2 * i + u, turn(v, 4 + 8 * (2 * i + u)), sides)
                if i % 2 == 0:
                    at = X_MID + 8 * i + 8 * u
                    other = turn(mid[m0 + i + 1, 8 * u : 8 * u + 8, :], 64)
                    out[at : at + 8, :] = jnp.where(lane < 64, v, other)
        out[X_MID + 32 : X_MID + 40, :] = sides
        for i in range(2):
            out[X_FINE + NY * i : X_FINE + NY * (i + 1), :] = fine[f0 + i]
        packed = jnp.zeros((8, LANES), F32)
        boxes = jnp.zeros((8, LANES), F32)
        for t in range(4):
            v = ghost[32 * g0 + 8 * t : 32 * g0 + 8 * t + 8, :]
            packed = jnp.where(lane // 16 == t, turn(v, 16 * t + edge), packed)
            at = 32 * (t // 2) + 8 * (b0 + t % 2)
            boxes = jnp.where(lane // 32 == t, turn(bricks[at : at + 8, :], 32 * t + 2), boxes)
        out[X_GHOST : X_GHOST + 8, :] = packed
        out[X_BRICK : X_BRICK + 8, :] = boxes
    grp_even = lax.axis_index("grp") % 2 == 0
    xa[...] = jnp.where(grp_even, xr[...], xl[...])
    xb[...] = jnp.where(grp_even, xl[...], xr[...])


def sweep_all(
    fine, xa, xb, start, smid, sghost, bricks, mid_hbm, fin_hbm,
    v13, pext, coef, rep, m1, m2, xl, xr, mid_out, fin_out, xm, sems,
):
    grp = lax.axis_index("grp")
    even = grp % 2 == 0
    xl[...] = jnp.where(even, xb[...], xa[...])
    xr[...] = jnp.where(even, xa[...], xb[...])

    @pl.when(grp == 0)
    def _():
        xl[X_BRICK : X_BRICK + 8, :] = jnp.zeros((8, LANES), F32)

    @pl.when(grp == lax.axis_size("grp") - 1)
    def _():
        xr[X_BRICK : X_BRICK + 8, :] = jnp.zeros((8, LANES), F32)

    lane = iota((8, LANES), 1)
    ring = (lane < 18) | (lane >= 126)
    for field in range(2):
        pext[64 * field + 16 : 64 * field + 48, :] = bricks[32 * field : 32 * field + 32, :]
        for b in range(2):
            shift = -(32 * (2 * field + b) + 2)
            at = 64 * field + 8 * b
            pext[at : at + 8, :] = jnp.where(ring, turn(xl[X_BRICK : X_BRICK + 8, :], shift), 0.0)
            pext[at + 48 : at + 56, :] = jnp.where(ring, turn(xr[X_BRICK : X_BRICK + 8, :], shift), 0.0)
    b, l = iota((LANES, 3 * LANES), 0), iota((LANES, 3 * LANES), 1)
    z = l % LANES
    hit = (l < 128) & (b == jnp.where(z >= 96, z // 4 + 96, z // 4))
    hit = hit | ((l >= 128) & (l < 256) & (b == z // 8))
    hit = hit | ((l >= 256) & (b == jnp.where(z % 8 < 4, 127, 16)))
    spread = dot(pext[...], onehot(hit))
    coef[0:64, :] = spread[0:64] * (relaxation / 6.0)
    coef[64:128, :] = spread[64:128] * (1.0 / 36.0) - 0.5

    def inverse13(bx):
        return coef[8 * (bx + 2) : 8 * (bx + 3), 0:LANES]

    def weight13(bx):
        return coef[64 + 8 * (bx + 2) : 72 + 8 * (bx + 2), 0:LANES]

    def inverse14(bx):
        return coef[8 * (bx + 2) : 8 * (bx + 3), LANES : 2 * LANES]

    def weight14(bx):
        return coef[64 + 8 * (bx + 2) : 72 + 8 * (bx + 2), LANES : 2 * LANES]

    for x in range(-5, 21):
        q = x // 2
        if q < 0:
            v = xl[X_START + 8 * (q + 3) : X_START + 8 * (q + 4), :]
        elif q > 7:
            v = xr[X_START + 8 * (q - 8) : X_START + 8 * (q - 7), :]
        else:
            v = start[8 * q : 8 * q + 8, :]
        v = jnp.where(inverse13(x // 4) != 0.0, v, 0.0)
        v13[x + 5, 0:8, :] = v
        v13[x + 5, 8:16, :] = v

    for base, edge in ((0, xl), (4, xr)):
        sides = edge[X_MID + 32 : X_MID + 40, :]
        for i in range(4):
            for u in range(2):
                at = X_MID + 16 * (i // 2) + 8 * u
                v = turn(edge[at : at + 8, :], 64 * (i % 2))
                xm[base + i, 8 * u : 8 * u + 8, :] = jnp.where(lane < 64, v, turn(sides, -(4 + 8 * (2 * i + u))))

    def rhs13(x, u):
        if x < 0:
            return xm[x + 4, 8 * u : 8 * u + 8, :]
        if x > 15:
            return xm[x - 12, 8 * u : 8 * u + 8, :]
        return smid[x, 8 * u : 8 * u + 8, :]

    for n in range(SWEEPS):
        low, high = -4 + n, 19 - n
        planes = {}
        for x in range(low - 1, high + 2):
            tiles = [v13[x + 5, 8 * u : 8 * u + 8, :] for u in range(2)]
            planes[x] = along_y(tiles, [turn(v, 1) + turn(v, -1) for v in tiles])
            if x > low:
                o = x - 1
                for u in range(2):
                    d = along_x(planes[o - 1][0][u], planes[o][0][u], planes[x][0][u])
                    e = along_x(planes[o - 1][1][u], planes[o][1][u], planes[x][1][u])
                    v13[o + 5, 8 * u : 8 * u + 8, :] = relax(
                        v13[o + 5, 8 * u : 8 * u + 8, :],
                        rhs13(o, u), inverse13(o // 4), weight13(o // 4), d, e, planes[o][1][u],
                    )
    for x in range(16):
        for u in range(2):
            mid_out[x, pl.ds(u, 8, 2), :] = v13[x + 5, 8 * u : 8 * u + 8, 0:64]
    mid_copy = pltpu.make_async_copy(mid_out, mid_hbm, sems.at[0])
    mid_copy.start()

    b, l = iota((LANES, 3 * LANES), 0), iota((LANES, 3 * LANES), 1)
    j = l % 8
    hit = (l < 128) & (b == l // 2)
    hit = hit | ((l >= 128) & (l < 256) & (b == jnp.where(j < 4, 126 + j // 2, 62 + j // 2)))
    hit = hit | ((l >= 256) & (b == jnp.where(j < 4, 63, 0)))
    parents = jnp.concatenate(
        [
            jnp.where(inverse13(x // 4) != 0.0, v13[x + 5, 8 * u : 8 * u + 8, :], 0.0)
            for x in range(-2, 18)
            for u in range(2)
        ],
        axis=0,
    )
    rep[...] = dot(parents, onehot(hit))

    def parent(q, u):
        return rep[16 * (q + 2) + 8 * u : 16 * (q + 2) + 8 * u + 8, 0:LANES]

    zero = jnp.zeros((8, LANES), F32)
    halo = [[zero, zero] for _ in range(4)]
    for q in range(-2, 18):
        g, i = q // 8 + 1, q % 8
        for u in range(2):
            v = rep[16 * (q + 2) + 8 * u : 16 * (q + 2) + 8 * u + 8, LANES : 2 * LANES]
            halo[g][u] = jnp.where(lane // 16 == i, v, halo[g][u])
    halo = [[tiles[t // 2] for t in range(4)] for tiles in halo]
    halo_rhs, halo_inverse, halo_weight = [], [], []
    for g in range(4):
        if g == 0:
            packed = xl[X_GHOST : X_GHOST + 8, :]
            halo_rhs.append([turn(packed, 112 - 16 * t) for t in range(4)])
        elif g == 3:
            packed = xr[X_GHOST : X_GHOST + 8, :]
            halo_rhs.append([turn(packed, -16 * t) for t in range(4)])
        else:
            halo_rhs.append([sghost[32 * (g - 1) + 8 * t : 32 * (g - 1) + 8 * t + 8, :] for t in range(4)])
        for field, out in ((0, halo_inverse), (64, halo_weight)):
            one, two = (coef[field + 8 * (2 * g + k) : field + 8 * (2 * g + k) + 8, 2 * LANES :] for k in range(2))
            out.append(jnp.where(lane < 64, one, two))

    def z_main(v, halo_tile, i):
        edge = turn(halo_tile, -(8 * i + 4))
        return turn(jnp.where(lane == 127, edge, v), 1) + turn(jnp.where(lane == 0, edge, v), -1)

    def sweep_halo(halo, edges):
        planes = []
        for g in range(4):
            right = [jnp.where(lane % 8 == 3, e, v) for e, v in zip(edges[g], halo[g])]
            left = [jnp.where(lane % 8 == 4, e, v) for e, v in zip(edges[g], halo[g])]
            planes.append(along_y(halo[g], [turn(r, 1) + turn(v, -1) for r, v in zip(right, left)]))
        moved = [[[(turn(v, 8), turn(v, -8)) for v in part] for part in plane] for plane in planes]
        out = []
        for g in range(4):
            tiles = []
            for t in range(4):
                de = []
                for part in range(2):
                    before, after = moved[g][part][t]
                    if g > 0:
                        before = jnp.where(lane < 8, moved[g - 1][part][t][0], before)
                    if g < 3:
                        after = jnp.where(lane >= 120, moved[g + 1][part][t][1], after)
                    de.append(along_x(before, planes[g][part][t], after))
                tiles.append(
                    relax(
                        halo[g][t], halo_rhs[g][t], halo_inverse[g], halo_weight[g],
                        de[0], de[1], planes[g][1][t],
                    )
                )
            out.append(tiles)
        return out

    def rhs14(x, t):
        if x < 0:
            return xl[X_FINE + NY * (x + 2) + 8 * t : X_FINE + NY * (x + 2) + 8 * t + 8, :]
        if x > 31:
            return xr[X_FINE + NY * (x - 32) + 8 * t : X_FINE + NY * (x - 32) + 8 * t + 8, :]
        return fine[x, 8 * t : 8 * t + 8, :]

    edges = [[zero, zero] for _ in range(4)]
    for q in range(-2, 18):
        g, i = q // 8 + 1, q % 8
        for u in range(2):
            v = rep[16 * (q + 2) + 8 * u : 16 * (q + 2) + 8 * u + 8, 2 * LANES :]
            edges[g][u] = jnp.where(lane // 16 == i, v, edges[g][u])
    edges = [[tiles[t // 2] for t in range(4)] for tiles in edges]
    planes = {}
    for q in range(-2, 18):
        g, i = (2 * q) // 16 + 1, (2 * q) % 16
        tiles = [parent(q, u) for u in range(2)]
        sums = [z_main(tiles[u], halo[g][2 * u], i) for u in range(2)]
        planes[q] = along_y([tiles[t // 2] for t in range(4)], [sums[t // 2] for t in range(4)])
        o = q - 1
        if o >= -1:
            for t in range(4):
                f5, c5 = 5.0 * planes[o][0][t], 5.0 * planes[o][1][t]
                for child in range(2):
                    x, near = 2 * o + child, o - 1 + 2 * child
                    d, e = f5 + planes[near][0][t], c5 + planes[near][1][t]
                    m1[x + 3, 8 * t : 8 * t + 8, :] = relax(
                        parent(o, t // 2), rhs14(x, t), inverse14(x // 8), weight14(x // 8),
                        d, e, planes[o][1][t],
                    )
    halo = sweep_halo(halo, edges)

    pieces = []
    for n, source, target in ((1, m1, m2), (2, m2, None)):
        low, high = -2 + n, 33 - n
        if n == 1:
            edges = [[zero] * 4 for _ in range(4)]
            b, l = iota((LANES, LANES), 0), iota((LANES, LANES), 1)
            hit = ((b == 127) & (l % 8 == 3)) | ((b == 0) & (l % 8 == 4))
            wide = [source[x + 3] for x in range(low - 1, high + 2)]
            wide = dot(jnp.concatenate(wide, axis=0), onehot(hit))
            for x in range(low - 1, high + 2):
                g, i = x // 16 + 1, x % 16
                for t in range(4):
                    at = 32 * (x - low + 1) + 8 * t
                    edges[g][t] = jnp.where(lane // 8 == i, wide[at : at + 8], edges[g][t])
        planes = {}
        for x in range(low - 1, high + 2):
            g, i = x // 16 + 1, x % 16
            tiles = [source[x + 3, 8 * t : 8 * t + 8, :] for t in range(4)]
            planes[x] = along_y(tiles, [z_main(tiles[t], halo[g][t], i) for t in range(4)])
            if x > low:
                o = x - 1
                for t in range(4):
                    d = along_x(planes[o - 1][0][t], planes[o][0][t], planes[x][0][t])
                    e = along_x(planes[o - 1][1][t], planes[o][1][t], planes[x][1][t])
                    value = relax(
                        source[o + 3, 8 * t : 8 * t + 8, :],
                        rhs14(o, t), inverse14(o // 8), weight14(o // 8), d, e, planes[o][1][t],
                    )
                    if target is None:
                        fin_out[o, pl.ds(t, 8, 4), :] = value
                    else:
                        target[o + 3, 8 * t : 8 * t + 8, :] = value
                if target is None and o % 8 == 7:
                    part = pl.ds(o - 7, 8)
                    pieces.append(pltpu.make_async_copy(fin_out.at[part], fin_hbm.at[part], sems.at[1 + o // 8]))
                    pieces[-1].start()
        if n == 1:
            halo = sweep_halo(halo, edges)
    mid_copy.wait()
    for piece in pieces:
        piece.wait()


def pairing(couples):
    partner = {}
    for a, b in couples:
        partner[a], partner[b] = b, a
    return sorted(partner.items())


def pairings(groups, slabs):
    def at(g, s):
        return g * slabs + s

    every = range(groups)
    one = [(at(g, s), at(g, s + 1)) for g in every for s in range(0, slabs, 2)]
    two = [(at(g, s), at(g, s + 1)) for g in every for s in range(1, slabs - 1, 2)]
    two += [(at(g, s), at(g + 1, s)) for g in range(0, groups, 2) for s in (0, slabs - 1)]
    three = [(at(g, s), at(g, s + 2)) for g in every for s in range(slabs) if s % 4 < 2]
    four = [(at(g, s), at(g, s + 2)) for g in every for s in range(slabs - 2) if s % 4 >= 2]
    four += [(at(g, s), at(g, s + 1)) for g in every for s in (0, slabs - 2)]
    five = [(at(g, s), at(g + 1, s)) for g in range(0, groups, 2) for s in range(slabs)]
    six = [(at(g, s), at(g + 1, s)) for g in range(1, groups - 1, 2) for s in range(slabs)]
    six += [(at(g, s), at(g, s + 1)) for g in (0, groups - 1) for s in range(0, slabs, 2)]
    return [pairing(couples) for couples in (one, two, three, four, five, six)]


def build(mesh, interpret=False):
    one, two, three, four, five, six = pairings(mesh.shape["grp"], mesh.shape["slab"])

    def local(source, occupancy, classes, screen_table, parents, coarse):
        def sds(*shape):
            return jax.ShapeDtypeStruct(shape, F32)

        vm = pl.BlockSpec(memory_space=VMEM)
        sm = pl.BlockSpec(memory_space=SMEM)
        hbm = pl.BlockSpec(memory_space=pltpu.HBM)

        def swap(block, pairs):
            return lax.ppermute(block, ("grp", "slab"), pairs)

        za, zb, rows, pown, fine = pl.pallas_call(
            pack_z,
            out_shape=(
                sds(Z_ROWS, LANES), sds(Z_ROWS, LANES), sds(16, LANES), sds(64, LANES), sds(CX, NY, LANES),
            ),
            in_specs=[hbm] * 6,
            out_specs=(vm,) * 5,
            scratch_shapes=[
                VMEM((CX, NY, LANES), F32),
                VMEM((4, 4, 16), jnp.int32),
                VMEM((4, 4, 16), jnp.int32),
                SMEM((16,), F32),
                SMEM((2, 2, 8), jnp.int32),
                VMEM((1, 4, 512), F32),
                VMEM((Z_ROWS, LANES), F32),
                VMEM((Z_ROWS, LANES), F32),
                pltpu.SemaphoreType.DMA((6,)),
            ],
            interpret=interpret,
            compiler_params=pltpu.CompilerParams(vmem_limit_bytes=4 << 20),
            name="pack_z",
        )(*(pltpu.with_memory_space_constraint(x, pltpu.HBM) for x in (source, occupancy, classes, screen_table, parents, coarse)))
        ha = swap(za, one)
        hb = swap(zb, two)
        fc = swap(rows, three)
        fd = swap(rows, four)
        xa, xb, start, mid, ghost, bricks = pl.pallas_call(
            extend_z,
            out_shape=(
                sds(X_ROWS, LANES), sds(X_ROWS, LANES), sds(64, LANES), sds(16, 16, LANES),
                sds(64, LANES), sds(64, LANES),
            ),
            in_specs=[vm, sm] + [vm] * 6,
            out_specs=(vm,) * 6,
            scratch_shapes=[
                VMEM((24, 512), F32),
                VMEM((256, 2 * LANES), F32),
                VMEM((Z_ROWS, LANES), F32),
                VMEM((Z_ROWS, LANES), F32),
                VMEM((X_ROWS, LANES), F32),
                VMEM((X_ROWS, LANES), F32),
            ],
            interpret=interpret,
            compiler_params=pltpu.CompilerParams(vmem_limit_bytes=8 << 20),
            name="extend_z",
        )(fine, parents, coarse, pown, ha, hb, fc, fd)
        ga = swap(xa, five)
        gb = swap(xb, six)
        return pl.pallas_call(
            sweep_all,
            out_shape=(sds(16, 16, 64), sds(CX, NY, CZ)),
            in_specs=[vm] * 7,
            out_specs=(hbm, hbm),
            scratch_shapes=[
                VMEM((26, 16, LANES), F32),
                VMEM((LANES, LANES), F32),
                VMEM((LANES, 3 * LANES), F32),
                VMEM((320, 3 * LANES), F32),
                VMEM((38, NY, LANES), F32),
                VMEM((38, NY, LANES), F32),
                VMEM((X_ROWS, LANES), F32),
                VMEM((X_ROWS, LANES), F32),
                VMEM((16, 16, 64), F32),
                VMEM((CX, NY, LANES), F32),
                VMEM((8, 16, LANES), F32),
                pltpu.SemaphoreType.DMA((5,)),
            ],
            interpret=interpret,
            compiler_params=pltpu.CompilerParams(vmem_limit_bytes=16 << 20),
            name="sweep_all",
        )(fine, ga, gb, start, mid, ghost, bricks)

    return local


def solution(mesh, interpret=False):
    placed = (
        P("grp", None, "slab"),
        P("grp", None, "slab"),
        P("grp", None, "slab"),
        P(),
        P("grp", None, "slab"),
        P("grp", "slab", None),
    )
    return jax.shard_map(
        build(mesh, interpret),
        mesh=mesh,
        in_specs=placed,
        out_specs=(P("grp", None, "slab"), P("grp", None, "slab")),
        check_vma=False,
    )
```
